32 devices in a mesh: sfc: 8 (over z, x), grp: 4 (over y, core).
Axes of the slice: x: 2, y: 2, z: 4, core: 2. Of those that a mesh axis runs over, the one named last changes fastest.
Arguments:
- source: float32 [32, 16, 1024], P('sfc', None, 'grp'), may hold values from -8 to 8
- layer_counts: int32 [8], P('sfc'), may hold values from 1 to 4, 21 in all
Outputs:
- solution: float32 [32, 16, 1024], P('sfc', None, 'grp')
- residual: float32 [32, 16, 1024], P('sfc', None, 'grp')
- direction: float32 [32, 16, 1024], P('sfc', None, 'grp')
The draws below stay inside these ranges and needn't reach their ends.
Inputs may be any that keep to these rules, and one draw needn't show every extreme that they name: `layer_counts`: each entry counts the live leading slots of that index of sfc; they sum to 21, and at least one entry equals 4.
All inputs are finite; a program needn't handle non-finite values. No bound on the sum of `layer_counts` on one device may be relied on, other than what follows from the above.
Results may differ from the reference program's by a relative error of at most 0.00011.
Values sent between devices are 32-bit elements; how exact they have to be, the bound alone decides.
A program may use at most 64 MiB of HBM per device.

```python
import math
import jax
import jax.numpy as jnp
import numpy as np

E = 16
H = 8
BCAP = 4
PRE_SWEEPS = 2
POST_SWEEPS = 2
COARSE_SWEEPS = 4
SLOTS = 32
LIVE = 21
N_SFC = 8
N_GRP = 4


def draw_source(key, part):
    shape = (BCAP * N_SFC, E, N_GRP * E * E)
    slot = jnp.arange(BCAP * N_SFC, dtype=jnp.float32)
    device = jnp.floor(slot / BCAP)
    rise = (1.0 + 2.0 * device / max(N_SFC - 1, 1))[:, None, None]
    values = jax.random.normal(key, shape, jnp.float32) * rise
    return jnp.clip(values, -8.0, 8.0)


def profile(amount, total, reach, lean):
    portions = [(1 << 20) // math.isqrt(grade ** lean) + 1 for grade in range(2, amount + 1)]
    rest, given = total - reach - (amount - 1), [1] * (amount - 1)
    while rest > 0:
        free = [i for i in range(amount - 1) if given[i] < reach]
        whole, remaining = sum([portions[i] for i in free]), rest
        for i in free:
            extra = min(reach - given[i], max(1, remaining * portions[i] // whole), rest)
            given[i] = given[i] + extra
            rest = rest - extra
    return np.array([reach] + given)


def uneven_parts(own_key, amount, total, reach, slope):
    if amount == 2:
        one = jax.random.randint(own_key, (), max(1, total - reach), min(reach, total - 1) + 1)
        return jnp.stack([one, total - one])
    tallies = jnp.asarray(profile(amount, total, reach, slope), jnp.int32)
    twos = (amount - 1) // 2
    giver, sink = tallies[1:1 + 2 * twos:2], tallies[2:2 + 2 * twos:2]
    slack = jnp.minimum(giver - 1, reach - sink)
    shifted = jax.random.randint(jax.random.fold_in(own_key, 1), (twos,), 0, 1 << 20) % (slack + 1)
    tallies = tallies.at[1:1 + 2 * twos:2].set(giver - shifted).at[2:2 + 2 * twos:2].set(sink + shifted)
    return tallies[jax.random.permutation(jax.random.fold_in(own_key, 2), amount)]


def setup_inputs(seed: int = 0) -> dict:
    keys = jax.random.split(jax.random.key(seed), 3)
    return {
        "source": draw_source(jax.random.fold_in(keys[2], 71), 0),
        "layer_counts": uneven_parts(keys[1], N_SFC, LIVE, BCAP, 2).astype(jnp.int32),
    }


OMEGA = 2.0 / 3.0


def laplace(field, counts, edge):
    n_dev, planes, width = field.shape
    zero_plane = jnp.zeros((1, 1, width), jnp.float32)
    last_index = (counts * edge - 1).astype(jnp.int32)
    last = jnp.take_along_axis(field, last_index[:, None, None], axis=1)
    first = field[:, :1]
    prev_last = jnp.concatenate([zero_plane, last[:-1]], axis=0)
    next_first = jnp.concatenate([first[1:], zero_plane], axis=0)
    below = jnp.concatenate([prev_last, field[:, :-1]], axis=1)
    above = jnp.concatenate([field[:, 1:], jnp.zeros((n_dev, 1, width), jnp.float32)], axis=1)
    plane = jnp.arange(planes, dtype=jnp.int32)
    at_last = (plane[None, :] == last_index[:, None])[:, :, None]
    above = above + jnp.where(at_last, next_first, 0.0)
    pad_rows = jnp.zeros((n_dev, planes, edge), jnp.float32)
    north = jnp.concatenate([field[:, :, edge:], pad_rows], axis=2)
    south = jnp.concatenate([pad_rows, field[:, :, :-edge]], axis=2)
    column = (jnp.arange(width, dtype=jnp.int32) % edge)[None, None, :]
    pad_col = jnp.zeros((n_dev, planes, 1), jnp.float32)
    up_z = jnp.where(column != edge - 1, jnp.concatenate([field[:, :, 1:], pad_col], axis=2), 0.0)
    down_z = jnp.where(column != 0, jnp.concatenate([pad_col, field[:, :, :-1]], axis=2), 0.0)
    total = 6.0 * field - below - above - north - south - up_z - down_z
    live = (plane[None, :] < (counts * edge)[:, None])[:, :, None]
    return jnp.where(live, total, 0.0)


def restrict(field):
    n_dev, planes, width = field.shape
    across = width // (E * E) * E
    blocks = field.reshape(n_dev, planes // 2, 2, across // 2, 2, H, 2)
    return 0.125 * jnp.sum(blocks, axis=(2, 4, 6)).reshape(n_dev, planes // 2, (across // 2) * H)


def prolong(coarse):
    n_dev, planes, width = coarse.shape
    across = width // H
    blocks = coarse.reshape(n_dev, planes, 1, across, 1, H, 1)
    blocks = jnp.broadcast_to(blocks, (n_dev, planes, 2, across, 2, H, 2))
    return blocks.reshape(n_dev, planes * 2, across * 2 * H * 2)


def vcycle(rhs, counts):
    step = OMEGA / 6.0
    smooth = step * rhs
    for sweep in range(PRE_SWEEPS - 1):
        smooth = smooth + step * (rhs - laplace(smooth, counts, E))
    defect = rhs - laplace(smooth, counts, E)
    coarse_rhs = restrict(defect)
    coarse_step = OMEGA / 1.5
    correction = coarse_step * coarse_rhs
    for sweep in range(COARSE_SWEEPS - 1):
        correction = correction + coarse_step * (coarse_rhs - 0.25 * laplace(correction, counts, H))
    smooth = smooth + prolong(correction)
    for sweep in range(POST_SWEEPS):
        smooth = smooth + step * (rhs - laplace(smooth, counts, E))
    return smooth


def reference(source, layer_counts):
    width = source.shape[2]
    field = source.reshape(N_SFC, BCAP * E, width)
    plane = jnp.arange(BCAP * E, dtype=jnp.int32)
    live = (plane[None, :] < (layer_counts * E)[:, None])[:, :, None]
    first_rhs = jnp.where(live, field, 0.0)
    first_z = vcycle(first_rhs, layer_counts)
    image = laplace(first_z, layer_counts, E)
    rz_value = jnp.sum(first_rhs * first_z)
    curv = jnp.sum(first_z * image)
    alpha = rz_value / curv
    solution = alpha * first_z
    residual = first_rhs - alpha * image
    next_z = vcycle(residual, layer_counts)
    cross = jnp.sum(next_z * image)
    direction = next_z - (cross / curv) * first_z
    shape = (SLOTS, E, width)
    return solution.reshape(shape), residual.reshape(shape), direction.reshape(shape)
```

```python
import functools

import jax
import jax.numpy as jnp
import numpy as np
from jax import lax
from jax.experimental import pallas as pl
from jax.experimental.pallas import tpu as pltpu
from jax.sharding import PartitionSpec as P

MESH = pl.DeviceIdType.MESH
LANES = 128
SUBS = 8
STEP = 1.0 / 9.0
CSTEP = 4.0 / 9.0
WAYS = ((0, 1), (0, -1), (1, 0), (1, 1), (1, -1), (-1, 0), (-1, 1), (-1, -1))


def weights(edge):
    lane = np.arange(LANES)
    y, z = lane // edge, lane % edge

    def parts(y, z, last):
        dy, dz = y[None, :] - y[:, None], z[None, :] - z[:, None]
        one = 3.0 * ((dy == 0) & (dz == 0)) + ((dy == 0) & (abs(dz) == 1)) + ((abs(dy) == 1) & (dz == 0))
        down = 1.0 * ((dy == last) & (dz == 0))
        up = 1.0 * ((dy == -last) & (dz == 0))
        return one, down, up

    one, down, up = parts(y, z, SUBS - 1)
    two = one @ one + down @ up + up @ down
    side = down + up
    fine = [2 * one, 2 * side, two, one @ side + side @ one]
    one, down, up = parts(y // 2, z // 2, SUBS // 2 - 1)
    same = 1.0 * ((y[None, :] // 2 == y[:, None] // 2) & (z[None, :] // 2 == z[:, None] // 2))
    two = (one @ one + down @ up + up @ down) / 4
    down2, up2 = (one @ down + down @ one) / 4, (one @ up + up @ one) / 4
    three = (two @ one + down2 @ up + up2 @ down) / 4
    down3, up3 = (two @ down + down2 @ one) / 4, (two @ up + up2 @ one) / 4
    coarse = [same, one, two, three, down + up, down2 + up2, down3, up3]
    whole = np.concatenate(fine + coarse, axis=1)
    return whole.astype(jnp.bfloat16)


def split(x, pieces):
    out = []
    for i in range(pieces):
        part = x.astype(jnp.bfloat16)
        out.append(part)
        if i < pieces - 1:
            x = x - part.astype(jnp.float32)
    return out


def kernel(
    dims, count_hbm, source_hbm, weight_hbm, first_ref, image_ref, w_ref, source_out, scale_ref,
    source_ref, image_buf, counts, fine_w, coarse_w, rhs, pre, gather, other, coarse, ea, eb,
    mask, cmask, own, packed, side, below, above, part, red, local_sem,
    send_sem, recv_sem, red_sem, hello,
):
    slots, edge, tiles, n_sfc, n_grp = dims
    half = edge // 2
    planes = slots * edge
    rows, crows = (slots + 2) * edge, (slots + 2) * half
    wide = 3 * tiles
    mids = tuple(range(tiles - 1, 2 * tiles + 1))
    mine = tuple(range(tiles, 2 * tiles))
    f32 = jnp.float32
    sfc = lax.axis_index("sfc")
    grp = lax.axis_index("grp")
    me = sfc * n_grp + grp
    everyone = n_sfc * n_grp

    def there(ds, dg):
        flag = None
        if ds:
            flag = sfc < n_sfc - 1 if ds > 0 else sfc > 0
        if dg:
            extra = grp < n_grp - 1 if dg > 0 else grp > 0
            flag = extra if flag is None else jnp.logical_and(flag, extra)
        return flag

    gossip = n_sfc <= 9 and n_grp <= 4
    barrier = pltpu.get_barrier_semaphore()

    def place(i):
        peer = lax.rem(me + i, everyone)
        return peer, {"sfc": peer // n_grp, "grp": lax.rem(peer, n_grp)}

    def greet(i, carry):
        pl.semaphore_signal(barrier, inc=1, device_id=place(i)[1], device_id_type=MESH)
        return carry

    source_copy = pltpu.make_async_copy(source_hbm, source_ref, local_sem.at[1])
    count_copy = pltpu.make_async_copy(count_hbm, counts, local_sem.at[0])
    source_copy.start()
    count_copy.start()
    weight_copies = []
    for i, (ref, at, width) in enumerate(((fine_w, 0, 4 * LANES), (coarse_w, 4 * LANES, 8 * LANES))):
        for up in (0, 1):
            copy = pltpu.make_async_copy(
                weight_hbm.at[:, pl.ds(at, width)], ref.at[pl.ds(up * LANES, LANES), :],
                local_sem.at[2 + 2 * i + up],
            )
            copy.start()
            weight_copies.append(copy)
    if gossip:
        for ds, dg in WAYS:
            @pl.when(there(ds, dg))
            def _(ds=ds, dg=dg):
                pl.semaphore_signal(
                    barrier, inc=1, device_id={"sfc": sfc + ds, "grp": grp + dg},
                    device_id_type=MESH,
                )
    else:
        lax.fori_loop(1, everyone, greet, 0)

    def one(flag):
        return jnp.where(flag, 1, 0)

    def greet_far(rnd, far):
        if gossip and far < n_sfc:
            for ds in (far, -far):
                @pl.when(sfc + ds < n_sfc if ds > 0 else sfc + ds >= 0)
                def _(ds=ds):
                    pl.semaphore_signal(
                        hello.at[rnd], inc=1, device_id={"sfc": sfc + ds}, device_id_type=MESH
                    )

    def hear_far(rnd, far):
        if gossip and far < n_sfc:
            pl.semaphore_wait(hello.at[rnd], one(sfc + far < n_sfc) + one(sfc >= far))

    lane = lax.broadcasted_iota(jnp.int32, (SUBS, LANES), 1)
    low_half = lane < LANES // 2

    def has(flag_int):
        return flag_int > 0

    has_below = one(sfc > 0)
    has_above = one(sfc < n_sfc - 1)
    has_left = one(grp > 0)
    has_right = one(grp < n_grp - 1)

    zero = jnp.zeros((SUBS, LANES), f32)
    for ref in (rhs, pre, gather, other):
        for t in range(wide):
            ref[t, pl.ds(0, SUBS), :] = zero
            ref[t, pl.ds(SUBS + rows, SUBS), :] = zero
    for t in range(wide):
        for ref in (coarse, ea, eb):
            ref[t, pl.ds(0, SUBS), :] = zero
            ref[t, pl.ds(SUBS + crows, SUBS), :] = zero
    for t in range(wide):
        for at in (SUBS, rows):
            other[t, pl.ds(at, SUBS), :] = zero

    source_copy.wait()

    def copies(e, i, ds, dg, src):
        gpos = 1 - dg
        if ds == 0:
            source, target = src, side.at[e, gpos // 2]
        else:
            tile, amount = ((0, 2), (1, 3), (3, 2))[dg + 1]
            source = packed.at[e, int(ds > 0), pl.ds(tile, amount)]
            target = (below if ds > 0 else above).at[e, gpos, pl.ds(0, amount)]
        return pltpu.make_async_remote_copy(
            src_ref=source, dst_ref=target, send_sem=send_sem.at[i],
            recv_sem=recv_sem.at[e, i], device_id={"sfc": sfc + ds, "grp": grp + dg},
            device_id_type=MESH,
        )

    def start(e, src):
        for i, (ds, dg) in enumerate(WAYS):
            @pl.when(there(ds, dg))
            def _(i=i, ds=ds, dg=dg):
                copies(e, i, ds, dg, src).start()

    def receive(e, src):
        for i, (ds, dg) in enumerate(WAYS):
            @pl.when(there(-ds, -dg))
            def _(i=i, ds=ds, dg=dg):
                copies(e, i, ds, dg, src).wait_recv()

    def sent(e, src):
        for i, (ds, dg) in enumerate(WAYS):
            @pl.when(there(ds, dg))
            def _(i=i, ds=ds, dg=dg):
                copies(e, i, ds, dg, src).wait_send()

    def pack(e, src):
        cut = SUBS // 2
        for up in (0, 1):
            at = pl.ds(0, edge)
            value = [src[at, pl.ds(t * LANES, LANES)] for t in range(tiles)]
            if up:
                for s in range(1, slots):
                    at = pl.ds(s * edge, edge)
                    value = [
                        jnp.where(count > s, src[at, pl.ds(t * LANES, LANES)], value[t])
                        for t in range(tiles)
                    ]
            if up:
                near = [v[edge - SUBS :] for v in value]
                far = [v[edge - SUBS - cut : edge - SUBS] for v in value]
                edges = [v[edge - cut :] for v in value]
            else:
                near = [v[:SUBS] for v in value]
                far = [v[SUBS : SUBS + cut] for v in value]
                edges = [v[:cut] for v in value]
            packed[e, up, 0] = jnp.concatenate([far[0], edges[1]], axis=0)
            packed[e, up, 1] = near[0]
            packed[e, up, 2] = jnp.concatenate([far[0], far[1]], axis=0)
            packed[e, up, 3] = near[1]
            packed[e, up, 4] = jnp.concatenate([far[1], edges[0]], axis=0)

    def ghost(ref, e, up, g, h, t):
        cut = SUBS // 2
        near_h = 1 if up else 0
        if g == 1:
            if h == near_h:
                return ref[e, g, 0 if t == 0 else 2]
            mix, low = ref[e, g, 1], t == 0
        else:
            full = 1 if g == 0 else 0
            if h == near_h and t == full:
                return ref[e, g, 0 if g == 0 else 1]
            mix = ref[e, g, 1 if g == 0 else 0]
            if h == near_h:
                low = False
            elif t == full:
                low = True
            else:
                return jnp.zeros((SUBS, LANES), f32)
        part = mix[:cut] if low else mix[cut:]
        none = jnp.zeros((cut, LANES), f32)
        return jnp.concatenate([none, part] if up else [part, none], axis=0)

    def unpack(e, src):
        sides = ((0, has_left), (1, 1), (2, has_right))
        for g, present in sides:
            for s in range(slots + 2):
                for h in range(edge // SUBS):
                    for t in range(tiles):
                        cols = pl.ds(t * LANES, LANES)

                        def centre(slot):
                            at = pl.ds(slot * edge + h * SUBS, SUBS)
                            return src[at, cols] if g == 1 else side[e, g // 2, at, cols]

                        if s == 0:
                            value = jnp.where(has(has_below * present), ghost(below, e, 1, g, h, t), 0.0)
                        else:
                            up = one(count == s - 1) * has_above * present
                            value = jnp.zeros((SUBS, LANES), f32)
                            if s >= 2:
                                value = jnp.where(has(up), ghost(above, e, 0, g, h, t), value)
                            if s <= slots:
                                value = jnp.where(has(one(count >= s) * present), centre(s - 1), value)
                        rhs[g * tiles + t, pl.ds(SUBS + s * edge + h * SUBS, SUBS), :] = value

    def body(ref, t, first=0, n=rows):
        return ref[t, pl.ds(SUBS + first, n), :]

    def around(ref, t, first=0, n=rows):
        return ref[t, pl.ds(SUBS + first - 1, n), :] + ref[t, pl.ds(SUBS + first + 1, n), :]

    def spot(t):
        return t // tiles

    def product(values, pieces, w, width):
        n = values[0].shape[0]
        parts = [split(v, pieces) for v in values]
        pair = jnp.concatenate([jnp.concatenate(p[:2], axis=1) for p in parts], axis=0)
        out = jnp.dot(pair, w[:, pl.ds(0, width)], preferred_element_type=f32)
        if pieces == 3:
            last = jnp.concatenate([p[2] for p in parts], axis=0)
            out = out + jnp.dot(last, w[pl.ds(0, LANES), pl.ds(0, width)], preferred_element_type=f32)

        def get(i, k):
            return out[i * n : (i + 1) * n, k * LANES : (k + 1) * LANES]

        return get

    def halves(n):
        return jnp.broadcast_to(low_half[:1], (n, LANES))

    def cross(get, i, k, k_up, count_, n):
        none = jnp.zeros((n, LANES), f32)
        lower = get(i - 1, k_up) if i > 0 else none
        upper = get(i + 1, k) if i < count_ - 1 else none
        return lower, upper

    def blend(get, i, k, amount, n):
        lower, upper = cross(get, i, k, k, amount, n)
        return jnp.where(halves(n), lower, upper)

    low_wall = jnp.where(jnp.logical_and(lane < edge, grp == 0), 1.0, 0.0)
    high_wall = jnp.where(jnp.logical_and(lane >= LANES - edge, grp == n_grp - 1), 1.0, 0.0)

    def walls(value, x, t):
        n = value.shape[0]
        if t == mine[0]:
            value = value - x * jnp.broadcast_to(low_wall[:1], (n, LANES))
        if t == mine[-1]:
            value = value - x * jnp.broadcast_to(high_wall[:1], (n, LANES))
        return value

    def smooth():
        get = product([body(rhs, t) for t in range(wide)], 2, fine_w, 4 * LANES)
        seconds = []
        for t in range(wide):
            r = body(rhs, t)
            first = get(t, 0) + blend(get, t, 1, wide, rows)
            seconds.append(walls(get(t, 2) + blend(get, t, 3, wide, rows), r, t))
            near = around(rhs, t)
            pre[t, pl.ds(SUBS, rows), :] = 9.0 * r + near + 0.5 * first
            gather[t, pl.ds(SUBS, rows), :] = mask[1] * (first + near)
        for t in range(wide):
            other[t, pl.ds(SUBS, rows), :] = seconds[t] + around(gather, t)

    def reflect(q, high):
        turned = pltpu.roll(q, LANES // 2, 1)
        n = q.shape[0]
        at = lax.broadcasted_iota(jnp.int32, (n, LANES), 1) // (2 * edge)
        near, far = (1, 2) if high else (2, 1)
        return jnp.where(at == near, -turned, jnp.where(at == far, -q, 0.0))

    def correct():
        qs = []
        for t in range(wide):
            q = (
                other[t, pl.ds(SUBS, crows, stride=2), :] + other[t, pl.ds(SUBS + 1, crows, stride=2), :]
            )
            qs.append(cmask[spot(t)] * q)
        left, right = mids[0], mids[-1]
        qs[left] = jnp.where(has(has_left), qs[left], reflect(qs[mine[0]], False))
        qs[right] = jnp.where(has(has_right), qs[right], reflect(qs[mine[-1]], True))
        get = product(qs, 2, coarse_w, 8 * LANES)
        b0, b1, b2 = {}, {}, {}
        for t in mids:
            c = get(t, 0)
            j1 = get(t, 1) + blend(get, t, 4, wide, crows)
            j2 = get(t, 2) + blend(get, t, 5, wide, crows)
            j3 = get(t, 3) + (get(t - 1, 7) + get(t + 1, 6))
            coarse[t, pl.ds(SUBS, crows), :] = c
            b0[t] = 729.0 * c + 81.0 * j1 + (9.0 * j2 + j3)
            b1[t] = 81.0 * c + 18.0 * j1 + 3.0 * j2
            b2[t] = 9.0 * c + 3.0 * j1
        for t in mids:
            ea[t, pl.ds(SUBS, crows), :] = cmask[1] * (b2[t] + around(coarse, t, 0, crows))
        for t in mids:
            eb[t, pl.ds(SUBS, crows), :] = cmask[1] * (b1[t] + around(ea, t, 0, crows))
        return {t: b0[t] + around(eb, t, 0, crows) for t in mids}

    scale = CSTEP * STEP * STEP * STEP / 8.0
    square = STEP * STEP

    def tally(e):
        acc = zero
        for t in mine:
            r, q, v = (body(ref, t, edge, planes) for ref in (rhs, other, pre))
            acc = acc + jnp.sum((own[...] * (r + square * q) * v).reshape(-1, SUBS, LANES), axis=0)
            ce = coarse[t, pl.ds(SUBS + half, slots * half), :] * e[t][half : half + slots * half]
            ce = ce.reshape(slots, half // SUBS, SUBS, LANES).sum(axis=1)
            for s in range(slots):
                acc = acc + (0.25 * scale * square) * own[pl.ds(s * edge, SUBS), :] * ce[s]
        return square * acc

    def finish(e, again):
        low, n = SUBS, rows - 2 * SUBS
        for t in mids:
            for up in (0, 1):
                gather[t, pl.ds(SUBS + up, crows, stride=2), :] = e[t]
        for t in mids:
            other[t, pl.ds(SUBS + low, n), :] = mask[spot(t), pl.ds(low, n), :] * (
                body(pre, t, low, n) + scale * body(gather, t, low, n)
            )
        get = product([body(other, t, low, n) for t in mids], 3, fine_w, 4 * LANES)
        out = {}
        for i, t in enumerate(mids):
            first = get(i, 0) + blend(get, i, 1, len(mids), n)
            x = body(other, t, low, n)
            gather[t, pl.ds(SUBS + low, n), :] = mask[1, pl.ds(low, n), :] * (first + around(other, t, low, n))
        for i, t in enumerate(mids):
            if not again and t not in mine:
                continue
            x = body(other, t, low, n)
            second = walls(get(i, 2) + blend(get, i, 3, len(mids), n), x, t)
            out[t] = body(pre, t, low, n) + square * (second + around(gather, t, low, n))
        if again:
            for t in mids:
                gather[t, pl.ds(SUBS + low, n), :] = mask[spot(t), pl.ds(low, n), :] * out[t]
        skip = edge - low
        return [own[...] * out[t][skip : skip + planes] for t in mine]

    def laplace():
        get = product([body(gather, t, edge, planes) for t in mids], 3, fine_w, 2 * LANES)
        out = []
        for i, t in enumerate(mids):
            if t in mine:
                first = get(i, 0) + blend(get, i, 1, len(mids), planes)
                value = 9.0 * body(gather, t, edge, planes) - around(gather, t, edge, planes) - 0.5 * first
                out.append(square * (own[...] * value))
        return out

    count_copy.wait()
    count = counts[0]
    pack(0, source_ref)
    if gossip:
        near = (1 + one(sfc > 0) + one(sfc < n_sfc - 1)) * (1 + one(grp > 0) + one(grp < n_grp - 1))
        pl.semaphore_wait(barrier, near - 1)
    else:
        pl.semaphore_wait(barrier, everyone - 1)
    start(0, source_ref)

    for g, present in enumerate((has_left, 1, has_right)):
        for s in range(slots + 2):
            if s == 0:
                ok = has_below
            else:
                ok = one(count >= s) + one(count == s - 1) * has_above
            value = jnp.full((SUBS, LANES), ok * present, jnp.int32).astype(f32)
            for h in range(edge // SUBS):
                mask[g, pl.ds(s * edge + h * SUBS, SUBS), :] = value
            for h in range(half // SUBS):
                cmask[g, pl.ds(s * half + h * SUBS, SUBS), :] = value
    for s in range(slots):
        value = jnp.full((SUBS, LANES), one(count > s), jnp.int32).astype(f32)
        for h in range(edge // SUBS):
            own[pl.ds(s * edge + h * SUBS, SUBS), :] = value
    for copy in weight_copies:
        copy.wait()

    receive(0, source_ref)
    greet_far(0, 2)
    unpack(0, source_ref)
    smooth()
    firsts = finish(correct(), True)
    images = laplace()
    for i, value in enumerate(images):
        image_buf[:, pl.ds(i * LANES, LANES)] = value
    pack(1, image_buf)
    hear_far(0, 2)
    sent(0, source_ref)
    start(1, image_buf)
    acc_rz, acc_curv = zero, zero
    for i in range(tiles):
        cols = pl.ds(i * LANES, LANES)
        value = square * firsts[i]
        image = images[i]
        source = body(rhs, mine[i], edge, planes) * own[...]
        first_ref[:, cols] = value
        image_ref[:, cols] = image
        source_out[:, cols] = source
        acc_rz = acc_rz + jnp.sum((source * value).reshape(-1, SUBS, LANES), axis=0)
        acc_curv = acc_curv + jnp.sum((value * image).reshape(-1, SUBS, LANES), axis=0)
    row = lax.broadcasted_iota(jnp.int32, (1, LANES), 1)

    def whole(acc):
        return jnp.sum(jnp.sum(acc, axis=0, keepdims=True), axis=1, keepdims=True)

    rz, curv = whole(acc_rz), whole(acc_curv)
    known = jnp.where(row == 0, rz, jnp.where(row == 1, curv, 0.0))
    receive(1, image_buf)
    greet_far(1, 4)
    unpack(1, image_buf)

    def send(slot, device):
        return pltpu.make_async_remote_copy(
            src_ref=part, dst_ref=red.at[slot], send_sem=red_sem.at[0],
            recv_sem=red_sem.at[1], device_id=device, device_id_type=MESH,
        )

    smooth()
    e = correct()
    value = jnp.where(row == 2, whole(tally(e)), known)
    part[...] = value
    red[me] = value
    hear_far(1, 4)

    def go(i, carry):
        peer, device = place(i)
        send(me, device).start()
        return carry

    lax.fori_loop(1, everyone, go, 0)
    for i, value in enumerate(finish(e, False)):
        w_ref[:, pl.ds(i * LANES, LANES)] = square * value
    sent(1, image_buf)

    rest = red.at[pl.ds(0, everyone - 1)]
    pltpu.make_async_copy(rest, rest, red_sem.at[0]).wait()
    pltpu.make_async_copy(rest, rest, red_sem.at[1]).wait()
    sums = jnp.sum(red[...], axis=0)

    def pick(i):
        return jnp.sum(jnp.where(row == i, sums, 0.0), axis=1, keepdims=True)

    alpha = pick(0) / pick(1)
    ratio = pick(2) / pick(1)
    scale_ref[...] = jnp.concatenate(
        [jnp.broadcast_to(alpha, (1, LANES)), jnp.broadcast_to(ratio, (1, LANES))], axis=0
    )


def combine(first, image, w, source, scale, solution_ref, residual_ref, direction_ref):
    alpha = scale[0:1, 0:1]
    ratio = scale[1:2, 0:1]
    solution_ref[...] = alpha * first[...]
    residual_ref[...] = source[...] - alpha * image[...]
    direction_ref[...] = alpha * (ratio * first[...] - w[...])


def shards(n_sfc, n_grp, source, layer_counts):
    slots, edge, width = source.shape
    planes, tiles = slots * edge, width // LANES
    rows, crows = (slots + 2) * edge, (slots + 2) * edge // 2
    f32 = jnp.float32
    vmem = pltpu.VMEM
    dma = pltpu.SemaphoreType.DMA
    n = n_sfc * n_grp
    out = jax.ShapeDtypeStruct((planes, width), f32)
    fine = vmem((3 * tiles, rows + 2 * SUBS, LANES), f32)
    coarse = vmem((3 * tiles, crows + 2 * SUBS, LANES), f32)
    parts = pl.pallas_call(
        functools.partial(kernel, (slots, edge, tiles, n_sfc, n_grp)),
        out_shape=(out, out, out, out, jax.ShapeDtypeStruct((2, LANES), f32)),
        in_specs=[pl.BlockSpec(memory_space=pltpu.HBM)] * 3,
        out_specs=[pl.BlockSpec(memory_space=pltpu.VMEM)] * 5,
        scratch_shapes=[
            vmem((planes, width), f32),
            vmem((planes, width), f32),
            pltpu.SMEM((1,), jnp.int32),
            vmem((2 * LANES, 4 * LANES), jnp.bfloat16),
            vmem((2 * LANES, 8 * LANES), jnp.bfloat16),
            fine, fine, fine, fine, coarse, coarse, coarse,
            vmem((3, rows, LANES), f32),
            vmem((3, crows, LANES), f32),
            vmem((planes, LANES), f32),
            vmem((2, 2, 5, SUBS, LANES), f32),
            vmem((2, 2, planes, width), f32),
            vmem((2, 3, 3, SUBS, LANES), f32),
            vmem((2, 3, 3, SUBS, LANES), f32),
            vmem((1, LANES), f32),
            vmem((n, 1, LANES), f32),
            dma((6,)),
            dma((len(WAYS),)),
            dma((2, len(WAYS))),
            dma((2,)),
            pltpu.SemaphoreType.REGULAR((2,)),
        ],
        compiler_params=pltpu.CompilerParams(
            collective_id=0, has_side_effects=True, vmem_limit_bytes=16 * 1024 * 1024
        ),
        name="pcg",
    )(layer_counts, source.reshape(planes, width), jnp.asarray(weights(edge)))
    outs = pl.pallas_call(
        combine,
        out_shape=(out, out, out),
        in_specs=[pl.BlockSpec(memory_space=pltpu.VMEM)] * 5,
        out_specs=[pl.BlockSpec(memory_space=pltpu.VMEM)] * 3,
        compiler_params=pltpu.CompilerParams(vmem_limit_bytes=16 * 1024 * 1024),
        name="combine",
    )(*parts)
    return tuple(o.reshape(source.shape) for o in outs)


def solution(mesh):
    n_sfc, n_grp = mesh.shape["sfc"], mesh.shape["grp"]
    return jax.shard_map(
        functools.partial(shards, n_sfc, n_grp),
        mesh=mesh,
        in_specs=(P("sfc", None, "grp"), P("sfc")),
        out_specs=(P("sfc", None, "grp"), P("sfc", None, "grp"), P("sfc", None, "grp")),
        check_vma=False,
    )
```

```python
import functools

import jax
import jax.numpy as jnp
import numpy as np
from jax import lax
from jax.experimental import pallas as pl
from jax.experimental.pallas import tpu as pltpu
from jax.sharding import PartitionSpec as P

MESH = pl.DeviceIdType.MESH
LANES = 128
SUBS = 8
STEP = 1.0 / 9.0
CSTEP = 4.0 / 9.0
WAYS = ((0, 1), (0, -1), (1, 0), (1, 1), (1, -1), (-1, 0), (-1, 1), (-1, -1))


def weights(edge):
    lane = np.arange(LANES)
    y, z = lane // edge, lane % edge

    def parts(y, z, last):
        dy, dz = y[None, :] - y[:, None], z[None, :] - z[:, None]
        one = 3.0 * ((dy == 0) & (dz == 0)) + ((dy == 0) & (abs(dz) == 1)) + ((abs(dy) == 1) & (dz == 0))
        down = 1.0 * ((dy == last) & (dz == 0))
        up = 1.0 * ((dy == -last) & (dz == 0))
        return one, down, up

    one, down, up = parts(y, z, SUBS - 1)
    two = one @ one + down @ up + up @ down
    side = down + up
    fine = [2 * one, 2 * side, two, one @ side + side @ one]
    one, down, up = parts(y // 2, z // 2, SUBS // 2 - 1)
    same = 1.0 * ((y[None, :] // 2 == y[:, None] // 2) & (z[None, :] // 2 == z[:, None] // 2))
    two = (one @ one + down @ up + up @ down) / 4
    down2, up2 = (one @ down + down @ one) / 4, (one @ up + up @ one) / 4
    three = (two @ one + down2 @ up + up2 @ down) / 4
    down3, up3 = (two @ down + down2 @ one) / 4, (two @ up + up2 @ one) / 4
    coarse = [same, one, two, three, down + up, down2 + up2, down3, up3]
    whole = np.concatenate(fine + coarse, axis=1)
    return whole.astype(jnp.bfloat16)


def split(x, pieces):
    out = []
    for i in range(pieces):
        part = x.astype(jnp.bfloat16)
        out.append(part)
        if i < pieces - 1:
            x = x - part.astype(jnp.float32)
    return out


def kernel(
    dims, count_hbm, source_hbm, weight_hbm, first_ref, image_ref, w_ref, source_out, scale_ref,
    source_ref, image_buf, counts, fine_w, coarse_w, rhs, pre, gather, other, coarse, ea, eb,
    mask, cmask, own, packed, side, below, above, part, red, local_sem,
    send_sem, recv_sem, red_sem, hello,
):
    slots, edge, tiles, n_sfc, n_grp = dims
    half = edge // 2
    planes = slots * edge
    rows, crows = (slots + 2) * edge, (slots + 2) * half
    wide = 3 * tiles
    mids = tuple(range(tiles - 1, 2 * tiles + 1))
    mine = tuple(range(tiles, 2 * tiles))
    f32 = jnp.float32
    sfc = lax.axis_index("sfc")
    grp = lax.axis_index("grp")
    me = sfc * n_grp + grp
    everyone = n_sfc * n_grp

    def there(ds, dg):
        flag = None
        if ds:
            flag = sfc < n_sfc - 1 if ds > 0 else sfc > 0
        if dg:
            extra = grp < n_grp - 1 if dg > 0 else grp > 0
            flag = extra if flag is None else jnp.logical_and(flag, extra)
        return flag

    gossip = n_sfc <= 9 and n_grp <= 4
    barrier = pltpu.get_barrier_semaphore()

    def place(i):
        peer = lax.rem(me + i, everyone)
        return peer, {"sfc": peer // n_grp, "grp": lax.rem(peer, n_grp)}

    def greet(i, carry):
        pl.semaphore_signal(barrier, inc=1, device_id=place(i)[1], device_id_type=MESH)
        return carry

    source_copy = pltpu.make_async_copy(source_hbm, source_ref, local_sem.at[1])
    source_copy.start()
    weight_copies = []
    for i, (ref, at, width) in enumerate(((fine_w, 0, 4 * LANES), (coarse_w, 4 * LANES, 8 * LANES))):
        for up in (0, 1):
            copy = pltpu.make_async_copy(
                weight_hbm.at[:, pl.ds(at, width)], ref.at[pl.ds(up * LANES, LANES), :],
                local_sem.at[2 + 2 * i + up],
            )
            copy.start()
            weight_copies.append(copy)
    if gossip:
        for ds, dg in WAYS:
            @pl.when(there(ds, dg))
            def _(ds=ds, dg=dg):
                pl.semaphore_signal(
                    barrier, inc=1, device_id={"sfc": sfc + ds, "grp": grp + dg},
                    device_id_type=MESH,
                )
    else:
        lax.fori_loop(1, everyone, greet, 0)

    def one(flag):
        return jnp.where(flag, 1, 0)

    rounds = (((2, 0), (-2, 0)), ((4, 0), (-4, 0)), ((0, 1), (0, -1)))

    def inside(ds, dg):
        flag = sfc + ds < n_sfc if ds >= 0 else sfc + ds >= 0
        return jnp.logical_and(flag, grp + dg < n_grp if dg >= 0 else grp + dg >= 0)

    def tell(rnd):
        if gossip:
            for ds, dg in rounds[rnd]:
                @pl.when(inside(ds, dg))
                def _(ds=ds, dg=dg):
                    pl.semaphore_signal(
                        hello.at[rnd], inc=1, device_id={"sfc": sfc + ds, "grp": grp + dg},
                        device_id_type=MESH,
                    )

    def hear(rnd):
        if gossip:
            pl.semaphore_wait(hello.at[rnd], sum(one(inside(ds, dg)) for ds, dg in rounds[rnd]))

    lane = lax.broadcasted_iota(jnp.int32, (SUBS, LANES), 1)
    low_half = lane < LANES // 2

    def has(flag_int):
        return flag_int > 0

    has_below = one(sfc > 0)
    has_above = one(sfc < n_sfc - 1)
    has_left = one(grp > 0)
    has_right = one(grp < n_grp - 1)

    zero = jnp.zeros((SUBS, LANES), f32)
    for ref in (rhs, pre, gather, other):
        for t in range(wide):
            ref[t, pl.ds(0, SUBS), :] = zero
            ref[t, pl.ds(SUBS + rows, SUBS), :] = zero
    for t in range(wide):
        for ref in (coarse, ea, eb):
            ref[t, pl.ds(0, SUBS), :] = zero
            ref[t, pl.ds(SUBS + crows, SUBS), :] = zero
    for t in range(wide):
        for at in (SUBS, rows):
            other[t, pl.ds(at, SUBS), :] = zero

    source_copy.wait()

    def copies(e, i, ds, dg, src):
        gpos = 1 - dg
        if ds == 0:
            source, target = src, side.at[e, gpos // 2]
        else:
            tile, amount = ((0, 2), (1, 3), (3, 2))[dg + 1]
            source = packed.at[e, int(ds > 0), pl.ds(tile, amount)]
            target = (below if ds > 0 else above).at[e, gpos, pl.ds(0, amount)]
        return pltpu.make_async_remote_copy(
            src_ref=source, dst_ref=target, send_sem=send_sem.at[i],
            recv_sem=recv_sem.at[e, i], device_id={"sfc": sfc + ds, "grp": grp + dg},
            device_id_type=MESH,
        )

    def start(e, src):
        for i, (ds, dg) in enumerate(WAYS):
            @pl.when(there(ds, dg))
            def _(i=i, ds=ds, dg=dg):
                copies(e, i, ds, dg, src).start()

    def receive(e, src):
        for i, (ds, dg) in enumerate(WAYS):
            @pl.when(there(-ds, -dg))
            def _(i=i, ds=ds, dg=dg):
                copies(e, i, ds, dg, src).wait_recv()

    def sent(e, src):
        for i, (ds, dg) in enumerate(WAYS):
            @pl.when(there(ds, dg))
            def _(i=i, ds=ds, dg=dg):
                copies(e, i, ds, dg, src).wait_send()

    def pack(e, src):
        cut = SUBS // 2
        for up in (0, 1):
            at = pl.ds(0, edge)
            value = [src[at, pl.ds(t * LANES, LANES)] for t in range(tiles)]
            if up:
                for s in range(1, slots):
                    at = pl.ds(s * edge, edge)
                    value = [
                        jnp.where(count > s, src[at, pl.ds(t * LANES, LANES)], value[t])
                        for t in range(tiles)
                    ]
            if up:
                near = [v[edge - SUBS :] for v in value]
                far = [v[edge - SUBS - cut : edge - SUBS] for v in value]
                edges = [v[edge - cut :] for v in value]
            else:
                near = [v[:SUBS] for v in value]
                far = [v[SUBS : SUBS + cut] for v in value]
                edges = [v[:cut] for v in value]
            packed[e, up, 0] = jnp.concatenate([far[0], edges[1]], axis=0)
            packed[e, up, 1] = near[0]
            packed[e, up, 2] = jnp.concatenate([far[0], far[1]], axis=0)
            packed[e, up, 3] = near[1]
            packed[e, up, 4] = jnp.concatenate([far[1], edges[0]], axis=0)

    def ghost(ref, e, up, g, h, t):
        cut = SUBS // 2
        near_h = 1 if up else 0
        if g == 1:
            if h == near_h:
                return ref[e, g, 0 if t == 0 else 2]
            mix, low = ref[e, g, 1], t == 0
        else:
            full = 1 if g == 0 else 0
            if h == near_h and t == full:
                return ref[e, g, 0 if g == 0 else 1]
            mix = ref[e, g, 1 if g == 0 else 0]
            if h == near_h:
                low = False
            elif t == full:
                low = True
            else:
                return jnp.zeros((SUBS, LANES), f32)
        part = mix[:cut] if low else mix[cut:]
        none = jnp.zeros((cut, LANES), f32)
        return jnp.concatenate([none, part] if up else [part, none], axis=0)

    def unpack(e, src):
        sides = ((0, has_left), (1, 1), (2, has_right))
        for g, present in sides:
            for s in range(slots + 2):
                for h in range(edge // SUBS):
                    for t in range(tiles):
                        cols = pl.ds(t * LANES, LANES)

                        def centre(slot):
                            at = pl.ds(slot * edge + h * SUBS, SUBS)
                            return src[at, cols] if g == 1 else side[e, g // 2, at, cols]

                        if s == 0:
                            value = jnp.where(has(has_below * present), ghost(below, e, 1, g, h, t), 0.0)
                        else:
                            up = one(count == s - 1) * has_above * present
                            value = jnp.zeros((SUBS, LANES), f32)
                            if s >= 2:
                                value = jnp.where(has(up), ghost(above, e, 0, g, h, t), value)
                            if s <= slots:
                                value = jnp.where(has(one(count >= s) * present), centre(s - 1), value)
                        rhs[g * tiles + t, pl.ds(SUBS + s * edge + h * SUBS, SUBS), :] = value

    def body(ref, t, first=0, n=rows):
        return ref[t, pl.ds(SUBS + first, n), :]

    def around(ref, t, first=0, n=rows):
        return ref[t, pl.ds(SUBS + first - 1, n), :] + ref[t, pl.ds(SUBS + first + 1, n), :]

    def spot(t):
        return t // tiles

    def product(values, pieces, w, width):
        n = values[0].shape[0]
        parts = [split(v, pieces) for v in values]
        pair = jnp.concatenate([jnp.concatenate(p[:2], axis=1) for p in parts], axis=0)
        out = jnp.dot(pair, w[:, pl.ds(0, width)], preferred_element_type=f32)
        if pieces == 3:
            last = jnp.concatenate([p[2] for p in parts], axis=0)
            out = out + jnp.dot(last, w[pl.ds(0, LANES), pl.ds(0, width)], preferred_element_type=f32)

        def get(i, k):
            return out[i * n : (i + 1) * n, k * LANES : (k + 1) * LANES]

        return get

    def halves(n):
        return jnp.broadcast_to(low_half[:1], (n, LANES))

    def cross(get, i, k, k_up, count_, n):
        none = jnp.zeros((n, LANES), f32)
        lower = get(i - 1, k_up) if i > 0 else none
        upper = get(i + 1, k) if i < count_ - 1 else none
        return lower, upper

    def blend(get, i, k, amount, n):
        lower, upper = cross(get, i, k, k, amount, n)
        return jnp.where(halves(n), lower, upper)

    low_wall = jnp.where(jnp.logical_and(lane < edge, grp == 0), 1.0, 0.0)
    high_wall = jnp.where(jnp.logical_and(lane >= LANES - edge, grp == n_grp - 1), 1.0, 0.0)

    def walls(value, x, t):
        n = value.shape[0]
        if t == mine[0]:
            value = value - x * jnp.broadcast_to(low_wall[:1], (n, LANES))
        if t == mine[-1]:
            value = value - x * jnp.broadcast_to(high_wall[:1], (n, LANES))
        return value

    def smooth():
        get = product([body(rhs, t) for t in range(wide)], 2, fine_w, 4 * LANES)
        seconds = []
        for t in range(wide):
            r = body(rhs, t)
            first = get(t, 0) + blend(get, t, 1, wide, rows)
            seconds.append(walls(get(t, 2) + blend(get, t, 3, wide, rows), r, t))
            near = around(rhs, t)
            pre[t, pl.ds(SUBS, rows), :] = 9.0 * r + near + 0.5 * first
            gather[t, pl.ds(SUBS, rows), :] = mask[1] * (first + near)
        for t in range(wide):
            other[t, pl.ds(SUBS, rows), :] = seconds[t] + around(gather, t)

    def reflect(q, high):
        turned = pltpu.roll(q, LANES // 2, 1)
        n = q.shape[0]
        at = lax.broadcasted_iota(jnp.int32, (n, LANES), 1) // (2 * edge)
        near, far = (1, 2) if high else (2, 1)
        return jnp.where(at == near, -turned, jnp.where(at == far, -q, 0.0))

    def correct():
        qs = []
        for t in range(wide):
            q = (
                other[t, pl.ds(SUBS, crows, stride=2), :] + other[t, pl.ds(SUBS + 1, crows, stride=2), :]
            )
            qs.append(cmask[spot(t)] * q)
        left, right = mids[0], mids[-1]
        qs[left] = jnp.where(has(has_left), qs[left], reflect(qs[mine[0]], False))
        qs[right] = jnp.where(has(has_right), qs[right], reflect(qs[mine[-1]], True))
        get = product(qs, 2, coarse_w, 8 * LANES)
        b0, b1, b2 = {}, {}, {}
        for t in mids:
            c = get(t, 0)
            j1 = get(t, 1) + blend(get, t, 4, wide, crows)
            j2 = get(t, 2) + blend(get, t, 5, wide, crows)
            j3 = get(t, 3) + (get(t - 1, 7) + get(t + 1, 6))
            coarse[t, pl.ds(SUBS, crows), :] = c
            b0[t] = 729.0 * c + 81.0 * j1 + (9.0 * j2 + j3)
            b1[t] = 81.0 * c + 18.0 * j1 + 3.0 * j2
            b2[t] = 9.0 * c + 3.0 * j1
        for t in mids:
            ea[t, pl.ds(SUBS, crows), :] = cmask[1] * (b2[t] + around(coarse, t, 0, crows))
        for t in mids:
            eb[t, pl.ds(SUBS, crows), :] = cmask[1] * (b1[t] + around(ea, t, 0, crows))
        return {t: b0[t] + around(eb, t, 0, crows) for t in mids}

    scale = CSTEP * STEP * STEP * STEP / 8.0
    square = STEP * STEP

    def tally(e):
        acc = zero
        for t in mine:
            r, q, v = (body(ref, t, edge, planes) for ref in (rhs, other, pre))
            acc = acc + jnp.sum((own[...] * (r + square * q) * v).reshape(-1, SUBS, LANES), axis=0)
            ce = coarse[t, pl.ds(SUBS + half, slots * half), :] * e[t][half : half + slots * half]
            ce = ce.reshape(slots, half // SUBS, SUBS, LANES).sum(axis=1)
            for s in range(slots):
                acc = acc + (0.25 * scale * square) * own[pl.ds(s * edge, SUBS), :] * ce[s]
        return square * acc

    def finish(e, again):
        low, n = SUBS, rows - 2 * SUBS
        for t in mids:
            for up in (0, 1):
                gather[t, pl.ds(SUBS + up, crows, stride=2), :] = e[t]
        for t in mids:
            other[t, pl.ds(SUBS + low, n), :] = mask[spot(t), pl.ds(low, n), :] * (
                body(pre, t, low, n) + scale * body(gather, t, low, n)
            )
        get = product([body(other, t, low, n) for t in mids], 3, fine_w, 4 * LANES)
        out = {}
        for i, t in enumerate(mids):
            first = get(i, 0) + blend(get, i, 1, len(mids), n)
            x = body(other, t, low, n)
            gather[t, pl.ds(SUBS + low, n), :] = mask[1, pl.ds(low, n), :] * (first + around(other, t, low, n))
        for i, t in enumerate(mids):
            if not again and t not in mine:
                continue
            x = body(other, t, low, n)
            second = walls(get(i, 2) + blend(get, i, 3, len(mids), n), x, t)
            out[t] = body(pre, t, low, n) + square * (second + around(gather, t, low, n))
        if again:
            for t in mids:
                gather[t, pl.ds(SUBS + low, n), :] = mask[spot(t), pl.ds(low, n), :] * out[t]
        skip = edge - low
        return [own[...] * out[t][skip : skip + planes] for t in mine]

    def laplace():
        get = product([body(gather, t, edge, planes) for t in mids], 3, fine_w, 2 * LANES)
        out = []
        for i, t in enumerate(mids):
            if t in mine:
                first = get(i, 0) + blend(get, i, 1, len(mids), planes)
                value = 9.0 * body(gather, t, edge, planes) - around(gather, t, edge, planes) - 0.5 * first
                out.append(square * (own[...] * value))
        return out

    count = count_hbm[0]
    pack(0, source_ref)
    if gossip:
        near = (1 + one(sfc > 0) + one(sfc < n_sfc - 1)) * (1 + one(grp > 0) + one(grp < n_grp - 1))
        pl.semaphore_wait(barrier, near - 1)
    else:
        pl.semaphore_wait(barrier, everyone - 1)
    start(0, source_ref)

    for g, present in enumerate((has_left, 1, has_right)):
        for s in range(slots + 2):
            if s == 0:
                ok = has_below
            else:
                ok = one(count >= s) + one(count == s - 1) * has_above
            value = jnp.full((SUBS, LANES), ok * present, jnp.int32).astype(f32)
            for h in range(edge // SUBS):
                mask[g, pl.ds(s * edge + h * SUBS, SUBS), :] = value
            for h in range(half // SUBS):
                cmask[g, pl.ds(s * half + h * SUBS, SUBS), :] = value
    for s in range(slots):
        value = jnp.full((SUBS, LANES), one(count > s), jnp.int32).astype(f32)
        for h in range(edge // SUBS):
            own[pl.ds(s * edge + h * SUBS, SUBS), :] = value
    for copy in weight_copies:
        copy.wait()

    receive(0, source_ref)
    tell(0)
    unpack(0, source_ref)
    smooth()
    firsts = finish(correct(), True)
    images = laplace()
    for i, value in enumerate(images):
        image_buf[:, pl.ds(i * LANES, LANES)] = value
    pack(1, image_buf)
    sent(0, source_ref)
    start(1, image_buf)
    hear(0)
    tell(1)
    acc_rz, acc_curv = zero, zero
    for i in range(tiles):
        cols = pl.ds(i * LANES, LANES)
        value = square * firsts[i]
        image = images[i]
        source = body(rhs, mine[i], edge, planes) * own[...]
        first_ref[:, cols] = value
        image_ref[:, cols] = image
        source_out[:, cols] = source
        acc_rz = acc_rz + jnp.sum((source * value).reshape(-1, SUBS, LANES), axis=0)
        acc_curv = acc_curv + jnp.sum((value * image).reshape(-1, SUBS, LANES), axis=0)
    row = lax.broadcasted_iota(jnp.int32, (1, LANES), 1)

    def whole(acc):
        return jnp.sum(jnp.sum(acc, axis=0, keepdims=True), axis=1, keepdims=True)

    rz, curv = whole(acc_rz), whole(acc_curv)
    known = jnp.where(row == 0, rz, jnp.where(row == 1, curv, 0.0))
    hear(1)
    tell(2)
    receive(1, image_buf)
    unpack(1, image_buf)

    def send(slot, device):
        return pltpu.make_async_remote_copy(
            src_ref=part, dst_ref=red.at[slot], send_sem=red_sem.at[0],
            recv_sem=red_sem.at[1], device_id=device, device_id_type=MESH,
        )

    smooth()
    e = correct()
    value = jnp.where(row == 2, whole(tally(e)), known)
    part[...] = value
    red[me] = value
    hear(2)

    if everyone <= 64:
        turn = jnp.where(2 * sfc >= n_sfc, 1, n_sfc - 1)
        grps = [lax.rem(grp + i, n_grp) for i in range(n_grp)]
        for ds in (*range(1, n_sfc), 0):
            there_sfc = lax.rem(sfc + ds * turn, n_sfc)
            for dg in range(n_grp):
                if ds or dg:
                    send(me, {"sfc": there_sfc, "grp": grps[dg]}).start()
    else:
        def go(i, carry):
            peer, device = place(i)
            send(me, device).start()
            return carry

        lax.fori_loop(1, everyone, go, 0)
    for i, value in enumerate(finish(e, False)):
        w_ref[:, pl.ds(i * LANES, LANES)] = square * value
    sent(1, image_buf)

    rest = red.at[pl.ds(0, everyone - 1)]
    pltpu.make_async_copy(rest, rest, red_sem.at[0]).wait()
    pltpu.make_async_copy(rest, rest, red_sem.at[1]).wait()
    sums = jnp.sum(red[...], axis=0)

    def pick(i):
        return jnp.sum(jnp.where(row == i, sums, 0.0), axis=1, keepdims=True)

    alpha = pick(0) / pick(1)
    ratio = pick(2) / pick(1)
    scale_ref[...] = jnp.concatenate(
        [jnp.broadcast_to(alpha, (1, LANES)), jnp.broadcast_to(ratio, (1, LANES))], axis=0
    )


def combine(first, image, w, source, scale, solution_ref, residual_ref, direction_ref):
    alpha = scale[0:1, 0:1]
    ratio = scale[1:2, 0:1]
    solution_ref[...] = alpha * first[...]
    residual_ref[...] = source[...] - alpha * image[...]
    direction_ref[...] = alpha * (ratio * first[...] - w[...])


def shards(n_sfc, n_grp, source, layer_counts):
    slots, edge, width = source.shape
    planes, tiles = slots * edge, width // LANES
    rows, crows = (slots + 2) * edge, (slots + 2) * edge // 2
    f32 = jnp.float32
    vmem = pltpu.VMEM
    dma = pltpu.SemaphoreType.DMA
    n = n_sfc * n_grp
    out = jax.ShapeDtypeStruct((planes, width), f32)
    fine = vmem((3 * tiles, rows + 2 * SUBS, LANES), f32)
    coarse = vmem((3 * tiles, crows + 2 * SUBS, LANES), f32)
    parts = pl.pallas_call(
        functools.partial(kernel, (slots, edge, tiles, n_sfc, n_grp)),
        out_shape=(out, out, out, out, jax.ShapeDtypeStruct((2, LANES), f32)),
        in_specs=[pl.BlockSpec(memory_space=pltpu.SMEM)] + [pl.BlockSpec(memory_space=pltpu.HBM)] * 2,
        out_specs=[pl.BlockSpec(memory_space=pltpu.VMEM)] * 5,
        scratch_shapes=[
            vmem((planes, width), f32),
            vmem((planes, width), f32),
            pltpu.SMEM((1,), jnp.int32),
            vmem((2 * LANES, 4 * LANES), jnp.bfloat16),
            vmem((2 * LANES, 8 * LANES), jnp.bfloat16),
            fine, fine, fine, fine, coarse, coarse, coarse,
            vmem((3, rows, LANES), f32),
            vmem((3, crows, LANES), f32),
            vmem((planes, LANES), f32),
            vmem((2, 2, 5, SUBS, LANES), f32),
            vmem((2, 2, planes, width), f32),
            vmem((2, 3, 3, SUBS, LANES), f32),
            vmem((2, 3, 3, SUBS, LANES), f32),
            vmem((1, LANES), f32),
            vmem((n, 1, LANES), f32),
            dma((6,)),
            dma((len(WAYS),)),
            dma((2, len(WAYS))),
            dma((2,)),
            pltpu.SemaphoreType.REGULAR((3,)),
        ],
        compiler_params=pltpu.CompilerParams(
            collective_id=0, has_side_effects=True, vmem_limit_bytes=16 * 1024 * 1024
        ),
        name="pcg",
    )(layer_counts, pltpu.with_memory_space_constraint(source.reshape(planes, width), pltpu.HBM), pltpu.with_memory_space_constraint(jnp.asarray(weights(edge)), pltpu.HBM))
    outs = pl.pallas_call(
        combine,
        out_shape=(out, out, out),
        in_specs=[pl.BlockSpec(memory_space=pltpu.VMEM)] * 5,
        out_specs=[pl.BlockSpec(memory_space=pltpu.VMEM)] * 3,
        compiler_params=pltpu.CompilerParams(vmem_limit_bytes=16 * 1024 * 1024),
        name="combine",
    )(*parts)
    return tuple(o.reshape(source.shape) for o in outs)


def solution(mesh):
    n_sfc, n_grp = mesh.shape["sfc"], mesh.shape["grp"]
    return jax.shard_map(
        functools.partial(shards, n_sfc, n_grp),
        mesh=mesh,
        in_specs=(P("sfc", None, "grp"), P("sfc")),
        out_specs=(P("sfc", None, "grp"), P("sfc", None, "grp"), P("sfc", None, "grp")),
        check_vma=False,
    )
```

```python
import functools

import jax
import jax.numpy as jnp
import numpy as np
from jax import lax
from jax.experimental import pallas as pl
from jax.experimental.pallas import tpu as pltpu
from jax.sharding import PartitionSpec as P

MESH = pl.DeviceIdType.MESH
LANES = 128
SUBS = 8
STEP = 1.0 / 9.0
CSTEP = 4.0 / 9.0
WAYS = ((0, 1), (0, -1), (1, 0), (1, 1), (1, -1), (-1, 0), (-1, 1), (-1, -1))


def weights(edge):
    lane = np.arange(LANES)
    y, z = lane // edge, lane % edge

    def parts(y, z, last):
        dy, dz = y[None, :] - y[:, None], z[None, :] - z[:, None]
        one = 3.0 * ((dy == 0) & (dz == 0)) + ((dy == 0) & (abs(dz) == 1)) + ((abs(dy) == 1) & (dz == 0))
        down = 1.0 * ((dy == last) & (dz == 0))
        up = 1.0 * ((dy == -last) & (dz == 0))
        return one, down, up

    one, down, up = parts(y, z, SUBS - 1)
    two = one @ one + down @ up + up @ down
    side = down + up
    fine = [2 * one, 2 * side, two, one @ side + side @ one]
    one, down, up = parts(y // 2, z // 2, SUBS // 2 - 1)
    same = 1.0 * ((y[None, :] // 2 == y[:, None] // 2) & (z[None, :] // 2 == z[:, None] // 2))
    two = (one @ one + down @ up + up @ down) / 4
    down2, up2 = (one @ down + down @ one) / 4, (one @ up + up @ one) / 4
    three = (two @ one + down2 @ up + up2 @ down) / 4
    down3, up3 = (two @ down + down2 @ one) / 4, (two @ up + up2 @ one) / 4
    coarse = [same, one, two, three, down + up, down2 + up2, down3, up3]
    whole = np.concatenate(fine + coarse, axis=1)
    return whole.astype(jnp.bfloat16)


def split(x, pieces):
    out = []
    for i in range(pieces):
        part = x.astype(jnp.bfloat16)
        out.append(part)
        if i < pieces - 1:
            x = x - part.astype(jnp.float32)
    return out


def kernel(
    dims, count_hbm, source_hbm, weight_hbm, first_ref, image_ref, w_ref, source_out, scale_ref,
    source_ref, image_buf, weight_ref, rhs, pre, gather, other, coarse, ea, eb,
    mask, cmask, own, packed, side, below, above, part, red, dummy, local_sem,
    trade_sem, red_sem, hello,
):
    slots, edge, tiles, n_sfc, n_grp = dims
    half = edge // 2
    planes = slots * edge
    rows, crows = (slots + 2) * edge, (slots + 2) * half
    wide = 3 * tiles
    mids = tuple(range(tiles - 1, 2 * tiles + 1))
    mine = tuple(range(tiles, 2 * tiles))
    f32 = jnp.float32
    sfc = lax.axis_index("sfc")
    grp = lax.axis_index("grp")
    me = sfc * n_grp + grp
    everyone = n_sfc * n_grp

    def there(ds, dg):
        flag = None
        if ds:
            flag = sfc < n_sfc - 1 if ds > 0 else sfc > 0
        if dg:
            extra = grp < n_grp - 1 if dg > 0 else grp > 0
            flag = extra if flag is None else jnp.logical_and(flag, extra)
        return flag

    gossip = n_sfc <= 9 and n_grp <= 4
    barrier = pltpu.get_barrier_semaphore()

    def place(i):
        peer = lax.rem(me + i, everyone)
        return peer, {"sfc": peer // n_grp, "grp": lax.rem(peer, n_grp)}

    def greet(i, carry):
        pl.semaphore_signal(barrier, inc=1, device_id=place(i)[1], device_id_type=MESH)
        return carry

    source_copy = pltpu.make_async_copy(source_hbm, source_ref, local_sem.at[0])
    source_copy.start()
    for up in (0, 1):
        pltpu.make_async_copy(
            weight_hbm, weight_ref.at[pl.ds(up * LANES, LANES), :], local_sem.at[1]
        ).start()
    if gossip:
        for ds, dg in WAYS:
            @pl.when(there(ds, dg))
            def _(ds=ds, dg=dg):
                pl.semaphore_signal(
                    barrier, inc=1, device_id={"sfc": sfc + ds, "grp": grp + dg},
                    device_id_type=MESH,
                )
    else:
        lax.fori_loop(1, everyone, greet, 0)

    def one(flag):
        return jnp.where(flag, 1, 0)

    rounds = (((2, 0), (-2, 0)), ((4, 0), (-4, 0)), ((0, 1), (0, -1)))

    def inside(ds, dg):
        flag = sfc + ds < n_sfc if ds >= 0 else sfc + ds >= 0
        return jnp.logical_and(flag, grp + dg < n_grp if dg >= 0 else grp + dg >= 0)

    def tell(rnd):
        if gossip:
            for ds, dg in rounds[rnd]:
                @pl.when(inside(ds, dg))
                def _(ds=ds, dg=dg):
                    pl.semaphore_signal(
                        hello.at[rnd], inc=1, device_id={"sfc": sfc + ds, "grp": grp + dg},
                        device_id_type=MESH,
                    )

    def hear(rnd):
        if gossip:
            pl.semaphore_wait(hello.at[rnd], sum(one(inside(ds, dg)) for ds, dg in rounds[rnd]))

    lane = lax.broadcasted_iota(jnp.int32, (SUBS, LANES), 1)
    low_half = lane < LANES // 2

    def has(flag_int):
        return flag_int > 0

    has_below = one(sfc > 0)
    has_above = one(sfc < n_sfc - 1)
    has_left = one(grp > 0)
    has_right = one(grp < n_grp - 1)

    zero = jnp.zeros((SUBS, LANES), f32)
    for ref in (rhs, pre, gather, other):
        for t in range(wide):
            ref[t, pl.ds(0, SUBS), :] = zero
            ref[t, pl.ds(SUBS + rows, SUBS), :] = zero
    for t in range(wide):
        for ref in (coarse, ea, eb):
            ref[t, pl.ds(0, SUBS), :] = zero
            ref[t, pl.ds(SUBS + crows, SUBS), :] = zero
    for t in range(wide):
        for at in (SUBS, rows):
            other[t, pl.ds(at, SUBS), :] = zero

    source_copy.wait()

    def copies(e, ds, dg, src):
        gpos = 1 - dg
        if ds == 0:
            source, target = src, side.at[e, gpos // 2]
        else:
            tile, amount = ((0, 2), (1, 3), (3, 2))[dg + 1]
            source = packed.at[e, int(ds > 0), pl.ds(tile, amount)]
            target = (below if ds > 0 else above).at[e, gpos, pl.ds(0, amount)]
        return pltpu.make_async_remote_copy(
            src_ref=source, dst_ref=target, send_sem=trade_sem.at[0],
            recv_sem=trade_sem.at[1 + e], device_id={"sfc": sfc + ds, "grp": grp + dg},
            device_id_type=MESH,
        )

    def start(e, src):
        for ds, dg in WAYS:
            @pl.when(there(ds, dg))
            def _(ds=ds, dg=dg):
                copies(e, ds, dg, src).start()

    def settle(sem):
        column = slots * edge * tiles // SUBS
        for beside in range(3):
            for along in range(3):
                total = beside * column + along * (3 + 2 * beside)

                @pl.when(
                    jnp.logical_and(
                        has_left + has_right == beside, has_below + has_above == along
                    )
                )
                def _(total=total):
                    if total:
                        ref = dummy.at[pl.ds(0, total)]
                        pltpu.make_async_copy(ref, ref, trade_sem.at[sem]).wait()

    def pack(e, src):
        cut = SUBS // 2
        for up in (0, 1):
            at = pl.ds(0, edge)
            value = [src[at, pl.ds(t * LANES, LANES)] for t in range(tiles)]
            if up:
                for s in range(1, slots):
                    at = pl.ds(s * edge, edge)
                    value = [
                        jnp.where(count > s, src[at, pl.ds(t * LANES, LANES)], value[t])
                        for t in range(tiles)
                    ]
            if up:
                near = [v[edge - SUBS :] for v in value]
                far = [v[edge - SUBS - cut : edge - SUBS] for v in value]
                edges = [v[edge - cut :] for v in value]
            else:
                near = [v[:SUBS] for v in value]
                far = [v[SUBS : SUBS + cut] for v in value]
                edges = [v[:cut] for v in value]
            packed[e, up, 0] = jnp.concatenate([far[0], edges[1]], axis=0)
            packed[e, up, 1] = near[0]
            packed[e, up, 2] = jnp.concatenate([far[0], far[1]], axis=0)
            packed[e, up, 3] = near[1]
            packed[e, up, 4] = jnp.concatenate([far[1], edges[0]], axis=0)

    def ghost(ref, e, up, g, h, t):
        cut = SUBS // 2
        near_h = 1 if up else 0
        if g == 1:
            if h == near_h:
                return ref[e, g, 0 if t == 0 else 2]
            mix, low = ref[e, g, 1], t == 0
        else:
            full = 1 if g == 0 else 0
            if h == near_h and t == full:
                return ref[e, g, 0 if g == 0 else 1]
            mix = ref[e, g, 1 if g == 0 else 0]
            if h == near_h:
                low = False
            elif t == full:
                low = True
            else:
                return jnp.zeros((SUBS, LANES), f32)
        part = mix[:cut] if low else mix[cut:]
        none = jnp.zeros((cut, LANES), f32)
        return jnp.concatenate([none, part] if up else [part, none], axis=0)

    def unpack(e, src):
        sides = ((0, has_left), (1, 1), (2, has_right))
        for g, present in sides:
            for s in range(slots + 2):
                for h in range(edge // SUBS):
                    for t in range(tiles):
                        cols = pl.ds(t * LANES, LANES)

                        def centre(slot):
                            at = pl.ds(slot * edge + h * SUBS, SUBS)
                            return src[at, cols] if g == 1 else side[e, g // 2, at, cols]

                        if s == 0:
                            value = jnp.where(has(has_below * present), ghost(below, e, 1, g, h, t), 0.0)
                        else:
                            up = one(count == s - 1) * has_above * present
                            value = jnp.zeros((SUBS, LANES), f32)
                            if s >= 2:
                                value = jnp.where(has(up), ghost(above, e, 0, g, h, t), value)
                            if s <= slots:
                                value = jnp.where(has(one(count >= s) * present), centre(s - 1), value)
                        rhs[g * tiles + t, pl.ds(SUBS + s * edge + h * SUBS, SUBS), :] = value

    def body(ref, t, first=0, n=rows):
        return ref[t, pl.ds(SUBS + first, n), :]

    def around(ref, t, first=0, n=rows):
        return ref[t, pl.ds(SUBS + first - 1, n), :] + ref[t, pl.ds(SUBS + first + 1, n), :]

    def spot(t):
        return t // tiles

    def product(values, pieces, at, width):
        n = values[0].shape[0]
        parts = [split(v, pieces) for v in values]
        pair = jnp.concatenate([jnp.concatenate(p[:2], axis=1) for p in parts], axis=0)
        out = jnp.dot(pair, weight_ref[:, pl.ds(at, width)], preferred_element_type=f32)
        if pieces == 3:
            last = jnp.concatenate([p[2] for p in parts], axis=0)
            out = out + jnp.dot(last, weight_ref[pl.ds(0, LANES), pl.ds(at, width)], preferred_element_type=f32)

        def get(i, k):
            return out[i * n : (i + 1) * n, k * LANES : (k + 1) * LANES]

        return get

    def halves(n):
        return jnp.broadcast_to(low_half[:1], (n, LANES))

    def cross(get, i, k, k_up, count_, n):
        none = jnp.zeros((n, LANES), f32)
        lower = get(i - 1, k_up) if i > 0 else none
        upper = get(i + 1, k) if i < count_ - 1 else none
        return lower, upper

    def blend(get, i, k, amount, n):
        lower, upper = cross(get, i, k, k, amount, n)
        return jnp.where(halves(n), lower, upper)

    low_wall = jnp.where(jnp.logical_and(lane < edge, grp == 0), 1.0, 0.0)
    high_wall = jnp.where(jnp.logical_and(lane >= LANES - edge, grp == n_grp - 1), 1.0, 0.0)

    def walls(value, x, t):
        n = value.shape[0]
        if t == mine[0]:
            value = value - x * jnp.broadcast_to(low_wall[:1], (n, LANES))
        if t == mine[-1]:
            value = value - x * jnp.broadcast_to(high_wall[:1], (n, LANES))
        return value

    def smooth():
        get = product([body(rhs, t) for t in range(wide)], 2, 0, 4 * LANES)
        seconds = []
        for t in range(wide):
            r = body(rhs, t)
            first = get(t, 0) + blend(get, t, 1, wide, rows)
            seconds.append(walls(get(t, 2) + blend(get, t, 3, wide, rows), r, t))
            near = around(rhs, t)
            pre[t, pl.ds(SUBS, rows), :] = 9.0 * r + near + 0.5 * first
            gather[t, pl.ds(SUBS, rows), :] = mask[1] * (first + near)
        for t in range(wide):
            other[t, pl.ds(SUBS, rows), :] = seconds[t] + around(gather, t)

    def reflect(q, high):
        turned = pltpu.roll(q, LANES // 2, 1)
        n = q.shape[0]
        at = lax.broadcasted_iota(jnp.int32, (n, LANES), 1) // (2 * edge)
        near, far = (1, 2) if high else (2, 1)
        return jnp.where(at == near, -turned, jnp.where(at == far, -q, 0.0))

    def correct():
        qs = []
        for t in range(wide):
            q = (
                other[t, pl.ds(SUBS, crows, stride=2), :] + other[t, pl.ds(SUBS + 1, crows, stride=2), :]
            )
            qs.append(cmask[spot(t)] * q)
        left, right = mids[0], mids[-1]
        qs[left] = jnp.where(has(has_left), qs[left], reflect(qs[mine[0]], False))
        qs[right] = jnp.where(has(has_right), qs[right], reflect(qs[mine[-1]], True))
        get = product(qs, 2, 4 * LANES, 8 * LANES)
        b0, b1, b2 = {}, {}, {}
        for t in mids:
            c = get(t, 0)
            j1 = get(t, 1) + blend(get, t, 4, wide, crows)
            j2 = get(t, 2) + blend(get, t, 5, wide, crows)
            j3 = get(t, 3) + (get(t - 1, 7) + get(t + 1, 6))
            coarse[t, pl.ds(SUBS, crows), :] = c
            b0[t] = 729.0 * c + 81.0 * j1 + (9.0 * j2 + j3)
            b1[t] = 81.0 * c + 18.0 * j1 + 3.0 * j2
            b2[t] = 9.0 * c + 3.0 * j1
        for t in mids:
            ea[t, pl.ds(SUBS, crows), :] = cmask[1] * (b2[t] + around(coarse, t, 0, crows))
        for t in mids:
            eb[t, pl.ds(SUBS, crows), :] = cmask[1] * (b1[t] + around(ea, t, 0, crows))
        return {t: b0[t] + around(eb, t, 0, crows) for t in mids}

    scale = CSTEP * STEP * STEP * STEP / 8.0
    square = STEP * STEP

    def tally(e):
        acc = zero
        for t in mine:
            r, q, v = (body(ref, t, edge, planes) for ref in (rhs, other, pre))
            acc = acc + jnp.sum((own[...] * (r + square * q) * v).reshape(-1, SUBS, LANES), axis=0)
            ce = coarse[t, pl.ds(SUBS + half, slots * half), :] * e[t][half : half + slots * half]
            ce = ce.reshape(slots, half // SUBS, SUBS, LANES).sum(axis=1)
            for s in range(slots):
                acc = acc + (0.25 * scale * square) * own[pl.ds(s * edge, SUBS), :] * ce[s]
        return square * acc

    def finish(e, again):
        low, n = SUBS, rows - 2 * SUBS
        for t in mids:
            for up in (0, 1):
                gather[t, pl.ds(SUBS + up, crows, stride=2), :] = e[t]
        for t in mids:
            other[t, pl.ds(SUBS + low, n), :] = mask[spot(t), pl.ds(low, n), :] * (
                body(pre, t, low, n) + scale * body(gather, t, low, n)
            )
        get = product([body(other, t, low, n) for t in mids], 3, 0, 4 * LANES)
        out = {}
        for i, t in enumerate(mids):
            first = get(i, 0) + blend(get, i, 1, len(mids), n)
            x = body(other, t, low, n)
            gather[t, pl.ds(SUBS + low, n), :] = mask[1, pl.ds(low, n), :] * (first + around(other, t, low, n))
        for i, t in enumerate(mids):
            if not again and t not in mine:
                continue
            x = body(other, t, low, n)
            second = walls(get(i, 2) + blend(get, i, 3, len(mids), n), x, t)
            out[t] = body(pre, t, low, n) + square * (second + around(gather, t, low, n))
        if again:
            for t in mids:
                gather[t, pl.ds(SUBS + low, n), :] = mask[spot(t), pl.ds(low, n), :] * out[t]
        skip = edge - low
        return [own[...] * out[t][skip : skip + planes] for t in mine]

    def laplace():
        get = product([body(gather, t, edge, planes) for t in mids], 3, 0, 2 * LANES)
        out = []
        for i, t in enumerate(mids):
            if t in mine:
                first = get(i, 0) + blend(get, i, 1, len(mids), planes)
                value = 9.0 * body(gather, t, edge, planes) - around(gather, t, edge, planes) - 0.5 * first
                out.append(square * (own[...] * value))
        return out

    count = count_hbm[0]
    pack(0, source_ref)
    if gossip:
        near = (1 + one(sfc > 0) + one(sfc < n_sfc - 1)) * (1 + one(grp > 0) + one(grp < n_grp - 1))
        pl.semaphore_wait(barrier, near - 1)
    else:
        pl.semaphore_wait(barrier, everyone - 1)
    start(0, source_ref)

    for g, present in enumerate((has_left, 1, has_right)):
        for s in range(slots + 2):
            if s == 0:
                ok = has_below
            else:
                ok = one(count >= s) + one(count == s - 1) * has_above
            value = jnp.full((SUBS, LANES), ok * present, jnp.int32).astype(f32)
            for h in range(edge // SUBS):
                mask[g, pl.ds(s * edge + h * SUBS, SUBS), :] = value
            for h in range(half // SUBS):
                cmask[g, pl.ds(s * half + h * SUBS, SUBS), :] = value
    for s in range(slots):
        value = jnp.full((SUBS, LANES), one(count > s), jnp.int32).astype(f32)
        for h in range(edge // SUBS):
            own[pl.ds(s * edge + h * SUBS, SUBS), :] = value
    pltpu.make_async_copy(weight_ref, weight_ref, local_sem.at[1]).wait()

    settle(1)
    tell(0)
    unpack(0, source_ref)
    smooth()
    firsts = finish(correct(), True)
    images = laplace()
    for i, value in enumerate(images):
        image_buf[:, pl.ds(i * LANES, LANES)] = value
    pack(1, image_buf)
    settle(0)
    start(1, image_buf)
    hear(0)
    tell(1)
    acc_rz, acc_curv = zero, zero
    for i in range(tiles):
        cols = pl.ds(i * LANES, LANES)
        value = square * firsts[i]
        image = images[i]
        source = body(rhs, mine[i], edge, planes) * own[...]
        first_ref[:, cols] = value
        image_ref[:, cols] = image
        source_out[:, cols] = source
        acc_rz = acc_rz + jnp.sum((source * value).reshape(-1, SUBS, LANES), axis=0)
        acc_curv = acc_curv + jnp.sum((value * image).reshape(-1, SUBS, LANES), axis=0)
    row = lax.broadcasted_iota(jnp.int32, (1, LANES), 1)

    def whole(acc):
        return jnp.sum(jnp.sum(acc, axis=0, keepdims=True), axis=1, keepdims=True)

    rz, curv = whole(acc_rz), whole(acc_curv)
    known = jnp.where(row == 0, rz, jnp.where(row == 1, curv, 0.0))
    hear(1)
    tell(2)
    settle(2)
    unpack(1, image_buf)

    def send(slot, device):
        return pltpu.make_async_remote_copy(
            src_ref=part, dst_ref=red.at[slot], send_sem=red_sem.at[0],
            recv_sem=red_sem.at[1], device_id=device, device_id_type=MESH,
        )

    smooth()
    e = correct()
    value = jnp.where(row == 2, whole(tally(e)), known)
    part[...] = value
    red[me] = value
    hear(2)

    if everyone <= 64:
        turn = jnp.where(2 * sfc >= n_sfc, 1, n_sfc - 1)
        grps = [lax.rem(grp + i, n_grp) for i in range(n_grp)]
        for ds in (*range(1, n_sfc), 0):
            there_sfc = lax.rem(sfc + ds * turn, n_sfc)
            for dg in range(n_grp):
                if ds or dg:
                    send(me, {"sfc": there_sfc, "grp": grps[dg]}).start()
    else:
        def go(i, carry):
            peer, device = place(i)
            send(me, device).start()
            return carry

        lax.fori_loop(1, everyone, go, 0)
    for i, value in enumerate(finish(e, False)):
        w_ref[:, pl.ds(i * LANES, LANES)] = square * value
    settle(0)

    rest = red.at[pl.ds(0, everyone - 1)]
    pltpu.make_async_copy(rest, rest, red_sem.at[0]).wait()
    pltpu.make_async_copy(rest, rest, red_sem.at[1]).wait()
    sums = jnp.sum(red[...], axis=0)

    def pick(i):
        return jnp.sum(jnp.where(row == i, sums, 0.0), axis=1, keepdims=True)

    alpha = pick(0) / pick(1)
    ratio = pick(2) / pick(1)
    scale_ref[...] = jnp.concatenate(
        [jnp.broadcast_to(alpha, (1, LANES)), jnp.broadcast_to(ratio, (1, LANES))], axis=0
    )


def combine(first, image, w, source, scale, solution_ref, residual_ref, direction_ref):
    alpha = scale[0:1, 0:1]
    ratio = scale[1:2, 0:1]
    solution_ref[...] = alpha * first[...]
    residual_ref[...] = source[...] - alpha * image[...]
    direction_ref[...] = alpha * (ratio * first[...] - w[...])


def shards(n_sfc, n_grp, source, layer_counts):
    slots, edge, width = source.shape
    planes, tiles = slots * edge, width // LANES
    rows, crows = (slots + 2) * edge, (slots + 2) * edge // 2
    f32 = jnp.float32
    vmem = pltpu.VMEM
    dma = pltpu.SemaphoreType.DMA
    n = n_sfc * n_grp
    out = jax.ShapeDtypeStruct((planes, width), f32)
    fine = vmem((3 * tiles, rows + 2 * SUBS, LANES), f32)
    coarse = vmem((3 * tiles, crows + 2 * SUBS, LANES), f32)
    parts = pl.pallas_call(
        functools.partial(kernel, (slots, edge, tiles, n_sfc, n_grp)),
        out_shape=(out, out, out, out, jax.ShapeDtypeStruct((2, LANES), f32)),
        in_specs=[pl.BlockSpec(memory_space=pltpu.SMEM)] + [pl.BlockSpec(memory_space=pltpu.HBM)] * 2,
        out_specs=[pl.BlockSpec(memory_space=pltpu.VMEM)] * 5,
        scratch_shapes=[
            vmem((planes, width), f32),
            vmem((planes, width), f32),
            vmem((2 * LANES, 12 * LANES), jnp.bfloat16),
            fine, fine, fine, fine, coarse, coarse, coarse,
            vmem((3, rows, LANES), f32),
            vmem((3, crows, LANES), f32),
            vmem((planes, LANES), f32),
            vmem((2, 2, 5, SUBS, LANES), f32),
            vmem((2, 2, planes, width), f32),
            vmem((2, 3, 3, SUBS, LANES), f32),
            vmem((2, 3, 3, SUBS, LANES), f32),
            vmem((1, LANES), f32),
            vmem((n, 1, LANES), f32),
            vmem((2 * planes * tiles // SUBS + 14, SUBS, LANES), f32),
            dma((2,)),
            dma((3,)),
            dma((2,)),
            pltpu.SemaphoreType.REGULAR((3,)),
        ],
        compiler_params=pltpu.CompilerParams(
            collective_id=0, has_side_effects=True, vmem_limit_bytes=16 * 1024 * 1024
        ),
        name="pcg",
    )(layer_counts, pltpu.with_memory_space_constraint(source.reshape(planes, width), pltpu.HBM), pltpu.with_memory_space_constraint(jnp.asarray(weights(edge)), pltpu.HBM))
    outs = pl.pallas_call(
        combine,
        out_shape=(out, out, out),
        in_specs=[pl.BlockSpec(memory_space=pltpu.VMEM)] * 5,
        out_specs=[pl.BlockSpec(memory_space=pltpu.VMEM)] * 3,
        compiler_params=pltpu.CompilerParams(vmem_limit_bytes=16 * 1024 * 1024),
        name="combine",
    )(*parts)
    return tuple(o.reshape(source.shape) for o in outs)


def solution(mesh):
    n_sfc, n_grp = mesh.shape["sfc"], mesh.shape["grp"]
    return jax.shard_map(
        functools.partial(shards, n_sfc, n_grp),
        mesh=mesh,
        in_specs=(P("sfc", None, "grp"), P("sfc")),
        out_specs=(P("sfc", None, "grp"), P("sfc", None, "grp"), P("sfc", None, "grp")),
        check_vma=False,
    )
```

```python
import functools

import jax
import jax.numpy as jnp
import numpy as np
from jax import lax
from jax.experimental import pallas as pl
from jax.experimental.pallas import tpu as pltpu
from jax.sharding import PartitionSpec as P

MESH = pl.DeviceIdType.MESH
LANES = 128
SUBS = 8
STEP = 1.0 / 9.0
CSTEP = 4.0 / 9.0
WAYS = ((0, 1), (0, -1), (1, 0), (1, 1), (1, -1), (-1, 0), (-1, 1), (-1, -1))


def weights(edge):
    lane = np.arange(LANES)
    y, z = lane // edge, lane % edge

    def parts(y, z, last):
        dy, dz = y[None, :] - y[:, None], z[None, :] - z[:, None]
        one = 3.0 * ((dy == 0) & (dz == 0)) + ((dy == 0) & (abs(dz) == 1)) + ((abs(dy) == 1) & (dz == 0))
        down = 1.0 * ((dy == last) & (dz == 0))
        up = 1.0 * ((dy == -last) & (dz == 0))
        return one, down, up

    one, down, up = parts(y, z, SUBS - 1)
    two = one @ one + down @ up + up @ down
    side = down + up
    fine = [2 * one, 2 * side, two, one @ side + side @ one]
    one, down, up = parts(y // 2, z // 2, SUBS // 2 - 1)
    same = 1.0 * ((y[None, :] // 2 == y[:, None] // 2) & (z[None, :] // 2 == z[:, None] // 2))
    two = (one @ one + down @ up + up @ down) / 4
    down2, up2 = (one @ down + down @ one) / 4, (one @ up + up @ one) / 4
    three = (two @ one + down2 @ up + up2 @ down) / 4
    down3, up3 = (two @ down + down2 @ one) / 4, (two @ up + up2 @ one) / 4
    coarse = [same, one, two, three, down + up, down2 + up2, down3, up3]
    whole = np.concatenate(fine + coarse, axis=1)
    return whole.astype(jnp.bfloat16)


def split(x, pieces):
    out = []
    for i in range(pieces):
        part = x.astype(jnp.bfloat16)
        out.append(part)
        if i < pieces - 1:
            x = x - part.astype(jnp.float32)
    return out


def kernel(
    dims, count_hbm, source_hbm, weight_hbm, first_ref, image_ref, w_ref, source_out, scale_ref,
    source_ref, image_buf, weight_ref, rhs, pre, gather, other, dual, coarse, ea, eb,
    mask, cmask, own, packed, side, below, above, part, red, dummy, local_sem,
    trade_sem, red_sem, hello,
):
    slots, edge, tiles, n_sfc, n_grp = dims
    half = edge // 2
    planes = slots * edge
    rows, crows = (slots + 2) * edge, (slots + 2) * half
    wide = 3 * tiles
    mids = tuple(range(tiles - 1, 2 * tiles + 1))
    mine = tuple(range(tiles, 2 * tiles))
    f32 = jnp.float32
    sfc = lax.axis_index("sfc")
    grp = lax.axis_index("grp")
    me = sfc * n_grp + grp
    everyone = n_sfc * n_grp

    def there(ds, dg):
        flag = None
        if ds:
            flag = sfc < n_sfc - 1 if ds > 0 else sfc > 0
        if dg:
            extra = grp < n_grp - 1 if dg > 0 else grp > 0
            flag = extra if flag is None else jnp.logical_and(flag, extra)
        return flag

    gossip = n_sfc <= 9 and n_grp <= 4
    barrier = pltpu.get_barrier_semaphore()

    def place(i):
        peer = lax.rem(me + i, everyone)
        return peer, {"sfc": peer // n_grp, "grp": lax.rem(peer, n_grp)}

    def greet(i, carry):
        pl.semaphore_signal(barrier, inc=1, device_id=place(i)[1], device_id_type=MESH)
        return carry

    source_copy = pltpu.make_async_copy(source_hbm, source_ref, local_sem.at[0])
    source_copy.start()
    for up in (0, 1):
        pltpu.make_async_copy(
            weight_hbm, weight_ref.at[pl.ds(up * LANES, LANES), :], local_sem.at[1]
        ).start()
    if gossip:
        for ds, dg in WAYS:
            @pl.when(there(ds, dg))
            def _(ds=ds, dg=dg):
                pl.semaphore_signal(
                    barrier, inc=1, device_id={"sfc": sfc + ds, "grp": grp + dg},
                    device_id_type=MESH,
                )
    else:
        lax.fori_loop(1, everyone, greet, 0)

    def one(flag):
        return jnp.where(flag, 1, 0)

    rounds = (((2, 1), (2, -1), (-2, 1), (-2, -1), (0, 1), (0, -1)), ((4, 0), (-4, 0)))

    def inside(ds, dg):
        flag = sfc + ds < n_sfc if ds >= 0 else sfc + ds >= 0
        return jnp.logical_and(flag, grp + dg < n_grp if dg >= 0 else grp + dg >= 0)

    def tell(rnd):
        if gossip:
            for ds, dg in rounds[rnd]:
                @pl.when(inside(ds, dg))
                def _(ds=ds, dg=dg):
                    pl.semaphore_signal(
                        hello.at[rnd], inc=1, device_id={"sfc": sfc + ds, "grp": grp + dg},
                        device_id_type=MESH,
                    )

    def hear(rnd):
        if gossip:
            pl.semaphore_wait(hello.at[rnd], sum(one(inside(ds, dg)) for ds, dg in rounds[rnd]))

    lane = lax.broadcasted_iota(jnp.int32, (SUBS, LANES), 1)
    low_half = lane < LANES // 2

    def has(flag_int):
        return flag_int > 0

    has_below = one(sfc > 0)
    has_above = one(sfc < n_sfc - 1)
    has_left = one(grp > 0)
    has_right = one(grp < n_grp - 1)

    zero = jnp.zeros((SUBS, LANES), f32)
    for ref in (rhs, pre, gather, other):
        for t in range(wide):
            ref[t, pl.ds(0, SUBS), :] = zero
            ref[t, pl.ds(SUBS + rows, SUBS), :] = zero
    for t in range(wide):
        for ref in (coarse, ea, eb):
            ref[t, pl.ds(0, SUBS), :] = zero
            ref[t, pl.ds(SUBS + crows, SUBS), :] = zero
    for t in range(wide):
        for at in (SUBS, rows):
            other[t, pl.ds(at, SUBS), :] = zero

    source_copy.wait()

    def copies(e, ds, dg, src):
        gpos = 1 - dg
        if ds == 0:
            source, target = src, side.at[e, gpos // 2]
        else:
            tile, amount = ((0, 2), (1, 3), (3, 2))[dg + 1]
            source = packed.at[e, int(ds > 0), pl.ds(tile, amount)]
            target = (below if ds > 0 else above).at[e, gpos, pl.ds(0, amount)]
        return pltpu.make_async_remote_copy(
            src_ref=source, dst_ref=target, send_sem=trade_sem.at[0],
            recv_sem=trade_sem.at[1 + e], device_id={"sfc": sfc + ds, "grp": grp + dg},
            device_id_type=MESH,
        )

    def start(e, src):
        for ds, dg in WAYS:
            @pl.when(there(ds, dg))
            def _(ds=ds, dg=dg):
                copies(e, ds, dg, src).start()

    def settle(sem):
        column = slots * edge * tiles // SUBS
        for beside in range(3):
            for along in range(3):
                total = beside * column + along * (3 + 2 * beside)

                @pl.when(
                    jnp.logical_and(
                        has_left + has_right == beside, has_below + has_above == along
                    )
                )
                def _(total=total):
                    if total:
                        ref = dummy.at[pl.ds(0, total)]
                        pltpu.make_async_copy(ref, ref, trade_sem.at[sem]).wait()

    def pack(e, src):
        cut = SUBS // 2
        for up in (0, 1):
            at = pl.ds(0, edge)
            value = [src[at, pl.ds(t * LANES, LANES)] for t in range(tiles)]
            if up:
                for s in range(1, slots):
                    at = pl.ds(s * edge, edge)
                    value = [
                        jnp.where(count > s, src[at, pl.ds(t * LANES, LANES)], value[t])
                        for t in range(tiles)
                    ]
            if up:
                near = [v[edge - SUBS :] for v in value]
                far = [v[edge - SUBS - cut : edge - SUBS] for v in value]
                edges = [v[edge - cut :] for v in value]
            else:
                near = [v[:SUBS] for v in value]
                far = [v[SUBS : SUBS + cut] for v in value]
                edges = [v[:cut] for v in value]
            packed[e, up, 0] = jnp.concatenate([far[0], edges[1]], axis=0)
            packed[e, up, 1] = near[0]
            packed[e, up, 2] = jnp.concatenate([far[0], far[1]], axis=0)
            packed[e, up, 3] = near[1]
            packed[e, up, 4] = jnp.concatenate([far[1], edges[0]], axis=0)

    def ghost(ref, e, up, g, h, t):
        cut = SUBS // 2
        near_h = 1 if up else 0
        if g == 1:
            if h == near_h:
                return ref[e, g, 0 if t == 0 else 2]
            mix, low = ref[e, g, 1], t == 0
        else:
            full = 1 if g == 0 else 0
            if h == near_h and t == full:
                return ref[e, g, 0 if g == 0 else 1]
            mix = ref[e, g, 1 if g == 0 else 0]
            if h == near_h:
                low = False
            elif t == full:
                low = True
            else:
                return jnp.zeros((SUBS, LANES), f32)
        part = mix[:cut] if low else mix[cut:]
        none = jnp.zeros((cut, LANES), f32)
        return jnp.concatenate([none, part] if up else [part, none], axis=0)

    def unpack(e, src):
        sides = ((0, has_left), (1, 1), (2, has_right))
        for g, present in sides:
            for s in range(slots + 2):
                for h in range(edge // SUBS):
                    for t in range(tiles):
                        cols = pl.ds(t * LANES, LANES)

                        def centre(slot):
                            at = pl.ds(slot * edge + h * SUBS, SUBS)
                            return src[at, cols] if g == 1 else side[e, g // 2, at, cols]

                        if s == 0:
                            value = jnp.where(has(has_below * present), ghost(below, e, 1, g, h, t), 0.0)
                        else:
                            up = one(count == s - 1) * has_above * present
                            value = jnp.zeros((SUBS, LANES), f32)
                            if s >= 2:
                                value = jnp.where(has(up), ghost(above, e, 0, g, h, t), value)
                            if s <= slots:
                                value = jnp.where(has(one(count >= s) * present), centre(s - 1), value)
                        rhs[g * tiles + t, pl.ds(SUBS + s * edge + h * SUBS, SUBS), :] = value

    def body(ref, t, first=0, n=rows):
        return ref[t, pl.ds(SUBS + first, n), :]

    def around(ref, t, first=0, n=rows):
        return ref[t, pl.ds(SUBS + first - 1, n), :] + ref[t, pl.ds(SUBS + first + 1, n), :]

    def spot(t):
        return t // tiles

    def product(values, pieces, at, width):
        n = values[0].shape[0]
        parts = [split(v, pieces) for v in values]
        pair = jnp.concatenate([jnp.concatenate(p[:2], axis=1) for p in parts], axis=0)
        out = jnp.dot(pair, weight_ref[:, pl.ds(at, width)], preferred_element_type=f32)
        if pieces == 3:
            last = jnp.concatenate([p[2] for p in parts], axis=0)
            out = out + jnp.dot(last, weight_ref[pl.ds(0, LANES), pl.ds(at, width)], preferred_element_type=f32)

        def get(i, k):
            return out[i * n : (i + 1) * n, k * LANES : (k + 1) * LANES]

        return get

    def halves(n):
        return jnp.broadcast_to(low_half[:1], (n, LANES))

    def cross(get, i, k, k_up, count_, n):
        none = jnp.zeros((n, LANES), f32)
        lower = get(i - 1, k_up) if 0 < i <= count_ else none
        upper = get(i + 1, k) if -1 <= i < count_ - 1 else none
        return lower, upper

    def blend(get, i, k, amount, n):
        lower, upper = cross(get, i, k, k, amount, n)
        return jnp.where(halves(n), lower, upper)

    low_wall = jnp.where(jnp.logical_and(lane < edge, grp == 0), 1.0, 0.0)
    high_wall = jnp.where(jnp.logical_and(lane >= LANES - edge, grp == n_grp - 1), 1.0, 0.0)

    def walls(value, x, t):
        n = value.shape[0]
        if t == mine[0]:
            value = value - x * jnp.broadcast_to(low_wall[:1], (n, LANES))
        if t == mine[-1]:
            value = value - x * jnp.broadcast_to(high_wall[:1], (n, LANES))
        return value

    def smooth():
        get = product([body(rhs, t) for t in range(wide)], 2, 0, 4 * LANES)
        seconds = []
        for t in range(wide):
            r = body(rhs, t)
            first = get(t, 0) + blend(get, t, 1, wide, rows)
            seconds.append(walls(get(t, 2) + blend(get, t, 3, wide, rows), r, t))
            near = around(rhs, t)
            pre[t, pl.ds(SUBS, rows), :] = 9.0 * r + near + 0.5 * first
            gather[t, pl.ds(SUBS, rows), :] = mask[1] * (first + near)
        for t in range(wide):
            other[t, pl.ds(SUBS, rows), :] = seconds[t] + around(gather, t)

    def reflect(q, high):
        turned = pltpu.roll(q, LANES // 2, 1)
        n = q.shape[0]
        at = lax.broadcasted_iota(jnp.int32, (n, LANES), 1) // (2 * edge)
        near, far = (1, 2) if high else (2, 1)
        return jnp.where(at == near, -turned, jnp.where(at == far, -q, 0.0))

    def correct():
        qs = []
        for t in range(wide):
            q = (
                other[t, pl.ds(SUBS, crows, stride=2), :] + other[t, pl.ds(SUBS + 1, crows, stride=2), :]
            )
            qs.append(cmask[spot(t)] * q)
        left, right = mids[0], mids[-1]
        qs[left] = jnp.where(has(has_left), qs[left], reflect(qs[mine[0]], False))
        qs[right] = jnp.where(has(has_right), qs[right], reflect(qs[mine[-1]], True))
        get = product(qs, 2, 4 * LANES, 8 * LANES)
        b0, b1, b2 = {}, {}, {}
        for t in mids:
            c = get(t, 0)
            j1 = get(t, 1) + blend(get, t, 4, wide, crows)
            j2 = get(t, 2) + blend(get, t, 5, wide, crows)
            j3 = get(t, 3) + (get(t - 1, 7) + get(t + 1, 6))
            coarse[t, pl.ds(SUBS, crows), :] = c
            b0[t] = 729.0 * c + 81.0 * j1 + (9.0 * j2 + j3)
            b1[t] = 81.0 * c + 18.0 * j1 + 3.0 * j2
            b2[t] = 9.0 * c + 3.0 * j1
        for t in mids:
            ea[t, pl.ds(SUBS, crows), :] = cmask[1] * (b2[t] + around(coarse, t, 0, crows))
        for t in mids:
            eb[t, pl.ds(SUBS, crows), :] = cmask[1] * (b1[t] + around(ea, t, 0, crows))
        return {t: b0[t] + around(eb, t, 0, crows) for t in mids}

    scale = CSTEP * STEP * STEP * STEP / 8.0
    square = STEP * STEP

    def finish(e, outs, low, n):
        for t in mids:
            for up in (0, 1):
                gather[t, pl.ds(SUBS + up, crows, stride=2), :] = e[t]
        for t in mids:
            other[t, pl.ds(SUBS + low, n), :] = mask[spot(t), pl.ds(low, n), :] * (
                body(pre, t, low, n) + scale * body(gather, t, low, n)
            )
        get = product([body(other, t, low, n) for t in mids], 3, 0, 4 * LANES)
        first, out = mids[0], {}
        near = len(mids)
        for t in outs:
            i = t - first
            if t in mids:
                value = get(i, 0) + blend(get, i, 1, near, n) + around(other, t, low, n)
            else:
                value = blend(get, i, 1, near, n)
            gather[t, pl.ds(SUBS + low, n), :] = mask[1, pl.ds(low, n), :] * value
        for t in outs:
            i = t - first
            second = blend(get, i, 3, near, n)
            if t in mids:
                second = walls(get(i, 2) + second, body(other, t, low, n), t)
            out[t] = body(pre, t, low, n) + square * (second + around(gather, t, low, n))
        return out

    def owned(out, low):
        return [own[...] * out[t][edge - low : edge - low + planes] for t in mine]

    def laplace():
        get = product([body(gather, t, edge, planes) for t in mids], 3, 0, 2 * LANES)
        out = []
        for i, t in enumerate(mids):
            if t in mine:
                first = get(i, 0) + blend(get, i, 1, len(mids), planes)
                value = 9.0 * body(gather, t, edge, planes) - around(gather, t, edge, planes) - 0.5 * first
                out.append(square * (own[...] * value))
        return out

    count = count_hbm[0]
    pack(0, source_ref)
    if gossip:
        near = (1 + one(sfc > 0) + one(sfc < n_sfc - 1)) * (1 + one(grp > 0) + one(grp < n_grp - 1))
        pl.semaphore_wait(barrier, near - 1)
    else:
        pl.semaphore_wait(barrier, everyone - 1)
    start(0, source_ref)

    for g, present in enumerate((has_left, 1, has_right)):
        for s in range(slots + 2):
            if s == 0:
                ok = has_below
            else:
                ok = one(count >= s) + one(count == s - 1) * has_above
            value = jnp.full((SUBS, LANES), ok * present, jnp.int32).astype(f32)
            for h in range(edge // SUBS):
                mask[g, pl.ds(s * edge + h * SUBS, SUBS), :] = value
            for h in range(half // SUBS):
                cmask[g, pl.ds(s * half + h * SUBS, SUBS), :] = value
    for s in range(slots):
        value = jnp.full((SUBS, LANES), one(count > s), jnp.int32).astype(f32)
        for h in range(edge // SUBS):
            own[pl.ds(s * edge + h * SUBS, SUBS), :] = value
    pltpu.make_async_copy(weight_ref, weight_ref, local_sem.at[1]).wait()

    settle(1)
    tell(0)
    unpack(0, source_ref)
    smooth()
    low, n = SUBS, rows - 2 * SUBS
    out = finish(correct(), mids, low, n)
    for t in mids:
        gather[t, pl.ds(SUBS + low, n), :] = mask[spot(t), pl.ds(low, n), :] * out[t]
    firsts = owned(out, low)
    images = laplace()
    for i, value in enumerate(images):
        image_buf[:, pl.ds(i * LANES, LANES)] = value
    pack(1, image_buf)
    settle(0)
    start(1, image_buf)
    hear(0)
    tell(1)
    acc_rz, acc_curv = zero, zero
    for i in range(tiles):
        cols = pl.ds(i * LANES, LANES)
        value = square * firsts[i]
        image = images[i]
        source = body(rhs, mine[i], edge, planes) * own[...]
        first_ref[:, cols] = value
        image_ref[:, cols] = image
        source_out[:, cols] = source
        acc_rz = acc_rz + jnp.sum((source * value).reshape(-1, SUBS, LANES), axis=0)
        acc_curv = acc_curv + jnp.sum((value * image).reshape(-1, SUBS, LANES), axis=0)
    row = lax.broadcasted_iota(jnp.int32, (1, LANES), 1)

    def whole(acc):
        return jnp.sum(jnp.sum(acc, axis=0, keepdims=True), axis=1, keepdims=True)

    rz, curv = whole(acc_rz), whole(acc_curv)
    known = jnp.where(row == 0, rz, jnp.where(row == 1, curv, 0.0))

    for t in range(wide):
        if t in mine:
            rhs[t, pl.ds(SUBS, edge), :] = jnp.zeros((edge, LANES), f32)
            rhs[t, pl.ds(SUBS + edge, planes), :] = images[t - tiles]
            rhs[t, pl.ds(SUBS + edge + planes, edge), :] = jnp.zeros((edge, LANES), f32)
        else:
            rhs[t, pl.ds(SUBS, rows), :] = jnp.zeros((rows, LANES), f32)
    smooth()
    out = finish(correct(), range(wide), 0, rows)
    for t in range(wide):
        dual[t] = mask[spot(t)] * out[t]
    settle(2)
    unpack(1, image_buf)
    acc = zero
    for t in range(wide):
        acc = acc + jnp.sum((dual[t] * body(rhs, t)).reshape(-1, SUBS, LANES), axis=0)

    def send(slot, device):
        return pltpu.make_async_remote_copy(
            src_ref=part, dst_ref=red.at[slot], send_sem=red_sem.at[0],
            recv_sem=red_sem.at[1], device_id=device, device_id_type=MESH,
        )

    value = jnp.where(row == 2, whole(square * acc), known)
    part[...] = value
    red[me] = value
    hear(1)

    if everyone <= 64:
        turn = jnp.where(2 * sfc >= n_sfc, 1, n_sfc - 1)
        grps = [lax.rem(grp + i, n_grp) for i in range(n_grp)]
        for ds in (*range(1, n_sfc), 0):
            there_sfc = lax.rem(sfc + ds * turn, n_sfc)
            for dg in range(n_grp):
                if ds or dg:
                    send(me, {"sfc": there_sfc, "grp": grps[dg]}).start()
    else:
        def go(i, carry):
            peer, device = place(i)
            send(me, device).start()
            return carry

        lax.fori_loop(1, everyone, go, 0)
    smooth()
    for i, value in enumerate(owned(finish(correct(), mine, SUBS, rows - 2 * SUBS), SUBS)):
        w_ref[:, pl.ds(i * LANES, LANES)] = square * value
    settle(0)

    rest = red.at[pl.ds(0, everyone - 1)]
    pltpu.make_async_copy(rest, rest, red_sem.at[0]).wait()
    pltpu.make_async_copy(rest, rest, red_sem.at[1]).wait()
    sums = jnp.sum(red[...], axis=0)

    def pick(i):
        return jnp.sum(jnp.where(row == i, sums, 0.0), axis=1, keepdims=True)

    alpha = pick(0) / pick(1)
    ratio = pick(2) / pick(1)
    scale_ref[...] = jnp.concatenate(
        [jnp.broadcast_to(alpha, (1, LANES)), jnp.broadcast_to(ratio, (1, LANES))], axis=0
    )


def combine(first, image, w, source, scale, solution_ref, residual_ref, direction_ref):
    alpha = scale[0:1, 0:1]
    ratio = scale[1:2, 0:1]
    solution_ref[...] = alpha * first[...]
    residual_ref[...] = source[...] - alpha * image[...]
    direction_ref[...] = alpha * (ratio * first[...] - w[...])


def shards(n_sfc, n_grp, source, layer_counts):
    slots, edge, width = source.shape
    planes, tiles = slots * edge, width // LANES
    rows, crows = (slots + 2) * edge, (slots + 2) * edge // 2
    f32 = jnp.float32
    vmem = pltpu.VMEM
    dma = pltpu.SemaphoreType.DMA
    n = n_sfc * n_grp
    out = jax.ShapeDtypeStruct((planes, width), f32)
    fine = vmem((3 * tiles, rows + 2 * SUBS, LANES), f32)
    coarse = vmem((3 * tiles, crows + 2 * SUBS, LANES), f32)
    parts = pl.pallas_call(
        functools.partial(kernel, (slots, edge, tiles, n_sfc, n_grp)),
        out_shape=(out, out, out, out, jax.ShapeDtypeStruct((2, LANES), f32)),
        in_specs=[pl.BlockSpec(memory_space=pltpu.SMEM)] + [pl.BlockSpec(memory_space=pltpu.HBM)] * 2,
        out_specs=[pl.BlockSpec(memory_space=pltpu.VMEM)] * 5,
        scratch_shapes=[
            vmem((planes, width), f32),
            vmem((planes, width), f32),
            vmem((2 * LANES, 12 * LANES), jnp.bfloat16),
            fine, fine, fine, fine,
            vmem((3 * tiles, rows, LANES), f32),
            coarse, coarse, coarse,
            vmem((3, rows, LANES), f32),
            vmem((3, crows, LANES), f32),
            vmem((planes, LANES), f32),
            vmem((2, 2, 5, SUBS, LANES), f32),
            vmem((2, 2, planes, width), f32),
            vmem((2, 3, 3, SUBS, LANES), f32),
            vmem((2, 3, 3, SUBS, LANES), f32),
            vmem((1, LANES), f32),
            vmem((n, 1, LANES), f32),
            vmem((2 * planes * tiles // SUBS + 14, SUBS, LANES), f32),
            dma((2,)),
            dma((3,)),
            dma((2,)),
            pltpu.SemaphoreType.REGULAR((2,)),
        ],
        compiler_params=pltpu.CompilerParams(
            collective_id=0, has_side_effects=True, vmem_limit_bytes=16 * 1024 * 1024
        ),
        name="pcg",
    )(layer_counts, pltpu.with_memory_space_constraint(source.reshape(planes, width), pltpu.HBM), pltpu.with_memory_space_constraint(jnp.asarray(weights(edge)), pltpu.HBM))
    outs = pl.pallas_call(
        combine,
        out_shape=(out, out, out),
        in_specs=[pl.BlockSpec(memory_space=pltpu.VMEM)] * 5,
        out_specs=[pl.BlockSpec(memory_space=pltpu.VMEM)] * 3,
        compiler_params=pltpu.CompilerParams(vmem_limit_bytes=16 * 1024 * 1024),
        name="combine",
    )(*parts)
    return tuple(o.reshape(source.shape) for o in outs)


def solution(mesh):
    n_sfc, n_grp = mesh.shape["sfc"], mesh.shape["grp"]
    return jax.shard_map(
        functools.partial(shards, n_sfc, n_grp),
        mesh=mesh,
        in_specs=(P("sfc", None, "grp"), P("sfc")),
        out_specs=(P("sfc", None, "grp"), P("sfc", None, "grp"), P("sfc", None, "grp")),
        check_vma=False,
    )
```

```python
import functools

import jax
import jax.numpy as jnp
import numpy as np
from jax import lax
from jax.experimental import pallas as pl
from jax.experimental.pallas import tpu as pltpu
from jax.sharding import PartitionSpec as P

MESH = pl.DeviceIdType.MESH
LANES = 128
SUBS = 8
STEP = 1.0 / 9.0
CSTEP = 4.0 / 9.0
WAYS = ((1, 1), (1, -1), (-1, 1), (-1, -1), (1, 0), (-1, 0), (0, 1), (0, -1))


def weights(edge):
    lane = np.arange(LANES)
    y, z = lane // edge, lane % edge

    def parts(y, z, last):
        dy, dz = y[None, :] - y[:, None], z[None, :] - z[:, None]
        one = 3.0 * ((dy == 0) & (dz == 0)) + ((dy == 0) & (abs(dz) == 1)) + ((abs(dy) == 1) & (dz == 0))
        down = 1.0 * ((dy == last) & (dz == 0))
        up = 1.0 * ((dy == -last) & (dz == 0))
        return one, down, up

    one, down, up = parts(y, z, SUBS - 1)
    two = one @ one + down @ up + up @ down
    side = down + up
    fine = [2 * one, 2 * side, two, one @ side + side @ one]
    one, down, up = parts(y // 2, z // 2, SUBS // 2 - 1)
    same = 1.0 * ((y[None, :] // 2 == y[:, None] // 2) & (z[None, :] // 2 == z[:, None] // 2))
    two = (one @ one + down @ up + up @ down) / 4
    down2, up2 = (one @ down + down @ one) / 4, (one @ up + up @ one) / 4
    three = (two @ one + down2 @ up + up2 @ down) / 4
    down3, up3 = (two @ down + down2 @ one) / 4, (two @ up + up2 @ one) / 4
    coarse = [same, one, two, three, down + up, down2 + up2, down3, up3]
    whole = np.concatenate(fine + coarse, axis=1)
    return whole.astype(jnp.bfloat16)


def split(x, pieces):
    out = []
    for i in range(pieces):
        part = x.astype(jnp.bfloat16)
        out.append(part)
        if i < pieces - 1:
            x = x - part.astype(jnp.float32)
    return out


def kernel(
    dims, count_hbm, source_hbm, weight_hbm, first_ref, image_ref, w_ref, source_out, scale_ref,
    source_ref, image_buf, weight_ref, rhs, pre, gather, other, dual, coarse, ea, eb,
    mask, cmask, own, packed, side, below, above, part, red, dummy, local_sem,
    trade_sem, red_sem, hello,
):
    slots, edge, tiles, n_sfc, n_grp = dims
    half = edge // 2
    planes = slots * edge
    rows, crows = (slots + 2) * edge, (slots + 2) * half
    wide = 3 * tiles
    mids = tuple(range(tiles - 1, 2 * tiles + 1))
    mine = tuple(range(tiles, 2 * tiles))
    f32 = jnp.float32
    sfc = lax.axis_index("sfc")
    grp = lax.axis_index("grp")
    me = sfc * n_grp + grp
    everyone = n_sfc * n_grp

    def there(ds, dg):
        flag = None
        if ds:
            flag = sfc < n_sfc - 1 if ds > 0 else sfc > 0
        if dg:
            extra = grp < n_grp - 1 if dg > 0 else grp > 0
            flag = extra if flag is None else jnp.logical_and(flag, extra)
        return flag

    gossip = n_sfc <= 9 and n_grp <= 4
    barrier = pltpu.get_barrier_semaphore()

    def place(i):
        peer = lax.rem(me + i, everyone)
        return peer, {"sfc": peer // n_grp, "grp": lax.rem(peer, n_grp)}

    def greet(i, carry):
        pl.semaphore_signal(barrier, inc=1, device_id=place(i)[1], device_id_type=MESH)
        return carry

    if gossip:
        for ds, dg in WAYS:
            @pl.when(there(ds, dg))
            def _(ds=ds, dg=dg):
                pl.semaphore_signal(
                    barrier, inc=1, device_id={"sfc": sfc + ds, "grp": grp + dg},
                    device_id_type=MESH,
                )
    else:
        lax.fori_loop(1, everyone, greet, 0)

    source_copy = pltpu.make_async_copy(source_hbm, source_ref, local_sem.at[0])
    source_copy.start()
    for up in range(3):
        pltpu.make_async_copy(
            weight_hbm, weight_ref.at[pl.ds(up * LANES, LANES), :], local_sem.at[1]
        ).start()
    def one(flag):
        return jnp.where(flag, 1, 0)

    rounds = (((2, 1), (2, -1), (-2, 1), (-2, -1), (0, 1), (0, -1)), ((4, 0), (-4, 0)))

    def inside(ds, dg):
        flag = sfc + ds < n_sfc if ds >= 0 else sfc + ds >= 0
        return jnp.logical_and(flag, grp + dg < n_grp if dg >= 0 else grp + dg >= 0)

    def tell(rnd):
        if gossip:
            for ds, dg in rounds[rnd]:
                @pl.when(inside(ds, dg))
                def _(ds=ds, dg=dg):
                    pl.semaphore_signal(
                        hello.at[rnd], inc=1, device_id={"sfc": sfc + ds, "grp": grp + dg},
                        device_id_type=MESH,
                    )

    def hear(rnd):
        if gossip:
            pl.semaphore_wait(hello.at[rnd], sum(one(inside(ds, dg)) for ds, dg in rounds[rnd]))

    lane = lax.broadcasted_iota(jnp.int32, (SUBS, LANES), 1)
    low_half = lane < LANES // 2

    def has(flag_int):
        return flag_int > 0

    has_below = one(sfc > 0)
    has_above = one(sfc < n_sfc - 1)
    has_left = one(grp > 0)
    has_right = one(grp < n_grp - 1)

    zero = jnp.zeros((SUBS, LANES), f32)
    for ref in (rhs, pre, gather, other):
        for t in range(wide):
            ref[t, pl.ds(0, SUBS), :] = zero
            ref[t, pl.ds(SUBS + rows, SUBS), :] = zero
    for t in range(wide):
        for ref in (coarse, ea, eb):
            ref[t, pl.ds(0, SUBS), :] = zero
            ref[t, pl.ds(SUBS + crows, SUBS), :] = zero
    for t in range(wide):
        for at in (SUBS, rows):
            other[t, pl.ds(at, SUBS), :] = zero

    source_copy.wait()

    def copies(e, ds, dg, src):
        gpos = 1 - dg
        if ds == 0:
            source, target = src, side.at[e, gpos // 2]
        else:
            tile, amount = ((0, 2), (1, 3), (3, 2))[dg + 1]
            source = packed.at[e, int(ds > 0), pl.ds(tile, amount)]
            target = (below if ds > 0 else above).at[e, gpos, pl.ds(0, amount)]
        return pltpu.make_async_remote_copy(
            src_ref=source, dst_ref=target, send_sem=trade_sem.at[0],
            recv_sem=trade_sem.at[1 if e == 0 else 2 if (dg, ds) < (0, 0) else 3], device_id={"sfc": sfc + ds, "grp": grp + dg},
            device_id_type=MESH,
        )

    def start(e, src):
        for ds, dg in WAYS:
            @pl.when(there(ds, dg))
            def _(ds=ds, dg=dg):
                copies(e, ds, dg, src).start()

    column = slots * edge * tiles // SUBS
    ends, layers = has_left + has_right, has_below + has_above

    def settle(sem, amounts, times=1):
        for flags, tiles_in in amounts:
            if tiles_in:
                @pl.when(functools.reduce(jnp.logical_and, flags))
                def _(tiles_in=tiles_in):
                    ref = dummy.at[pl.ds(0, times * tiles_in)]
                    pltpu.make_async_copy(ref, ref, trade_sem.at[sem]).wait()

    def half_of(beside, along):
        return [
            ((beside == b, along == a, layers == l), b * (column + 2 * l) + 3 * a)
            for b in (0, 1) for l in (0, 1, 2) for a in (0, 1) if l - 1 <= a <= l
        ]

    both = [((ends == b, layers == l), b * (column + 2 * l) + 3 * l) for b in range(3) for l in range(3)]
    high, low_end = half_of(has_right, has_above), half_of(has_left, has_below)

    def pack(e, src):
        cut = SUBS // 2
        for up in (0, 1):
            at = pl.ds(0, edge)
            value = [src[at, pl.ds(t * LANES, LANES)] for t in range(tiles)]
            if up:
                for s in range(1, slots):
                    at = pl.ds(s * edge, edge)
                    value = [
                        jnp.where(count > s, src[at, pl.ds(t * LANES, LANES)], value[t])
                        for t in range(tiles)
                    ]
            if up:
                near = [v[edge - SUBS :] for v in value]
                far = [v[edge - SUBS - cut : edge - SUBS] for v in value]
                edges = [v[edge - cut :] for v in value]
            else:
                near = [v[:SUBS] for v in value]
                far = [v[SUBS : SUBS + cut] for v in value]
                edges = [v[:cut] for v in value]
            packed[e, up, 0] = jnp.concatenate([far[0], edges[1]], axis=0)
            packed[e, up, 1] = near[0]
            packed[e, up, 2] = jnp.concatenate([far[0], far[1]], axis=0)
            packed[e, up, 3] = near[1]
            packed[e, up, 4] = jnp.concatenate([far[1], edges[0]], axis=0)

    def ghost(ref, e, up, g, h, t):
        cut = SUBS // 2
        near_h = 1 if up else 0
        if g == 1:
            if h == near_h:
                return ref[e, g, 0 if t == 0 else 2]
            mix, low = ref[e, g, 1], t == 0
        else:
            full = 1 if g == 0 else 0
            if h == near_h and t == full:
                return ref[e, g, 0 if g == 0 else 1]
            mix = ref[e, g, 1 if g == 0 else 0]
            if h == near_h:
                low = False
            elif t == full:
                low = True
            else:
                return jnp.zeros((SUBS, LANES), f32)
        part = mix[:cut] if low else mix[cut:]
        none = jnp.zeros((cut, LANES), f32)
        return jnp.concatenate([none, part] if up else [part, none], axis=0)

    def unpack(e, src):
        sides = ((0, has_left), (1, 1), (2, has_right))
        for g, present in sides:
            for s in range(slots + 2):
                for h in range(edge // SUBS):
                    for t in range(tiles):
                        cols = pl.ds(t * LANES, LANES)

                        def centre(slot):
                            at = pl.ds(slot * edge + h * SUBS, SUBS)
                            return src[at, cols] if g == 1 else side[e, g // 2, at, cols]

                        if s == 0:
                            value = jnp.where(has(has_below * present), ghost(below, e, 1, g, h, t), 0.0)
                        else:
                            up = one(count == s - 1) * has_above * present
                            value = jnp.zeros((SUBS, LANES), f32)
                            if s >= 2:
                                value = jnp.where(has(up), ghost(above, e, 0, g, h, t), value)
                            if s <= slots:
                                value = jnp.where(has(one(count >= s) * present), centre(s - 1), value)
                        rhs[g * tiles + t, pl.ds(SUBS + s * edge + h * SUBS, SUBS), :] = value

    def body(ref, t, first=0, n=rows):
        return ref[t, pl.ds(SUBS + first, n), :]

    def around(ref, t, first=0, n=rows):
        return ref[t, pl.ds(SUBS + first - 1, n), :] + ref[t, pl.ds(SUBS + first + 1, n), :]

    def spot(t):
        return t // tiles

    def product(values, pieces, at, width):
        n = values[0].shape[0]
        parts = [split(v, pieces) for v in values]
        lhs = jnp.concatenate([jnp.concatenate(p, axis=1) for p in parts], axis=0)
        w = weight_ref[pl.ds(0, pieces * LANES), pl.ds(at, width)]
        out = jnp.dot(lhs, w, preferred_element_type=f32)

        def get(i, k):
            return out[i * n : (i + 1) * n, k * LANES : (k + 1) * LANES]

        return get

    def halves(n):
        return jnp.broadcast_to(low_half[:1], (n, LANES))

    def cross(get, i, k, k_up, count_, n):
        none = jnp.zeros((n, LANES), f32)
        lower = get(i - 1, k_up) if 0 < i <= count_ else none
        upper = get(i + 1, k) if -1 <= i < count_ - 1 else none
        return lower, upper

    def blend(get, i, k, amount, n):
        lower, upper = cross(get, i, k, k, amount, n)
        return jnp.where(halves(n), lower, upper)

    low_wall = jnp.where(jnp.logical_and(lane < edge, grp == 0), 1.0, 0.0)
    high_wall = jnp.where(jnp.logical_and(lane >= LANES - edge, grp == n_grp - 1), 1.0, 0.0)

    def walls(value, x, t):
        n = value.shape[0]
        if t == mine[0]:
            value = value - x * jnp.broadcast_to(low_wall[:1], (n, LANES))
        if t == mine[-1]:
            value = value - x * jnp.broadcast_to(high_wall[:1], (n, LANES))
        return value

    def smooth():
        get = product([body(rhs, t) for t in range(wide)], 2, 0, 4 * LANES)
        seconds = []
        for t in range(wide):
            r = body(rhs, t)
            first = get(t, 0) + blend(get, t, 1, wide, rows)
            seconds.append(walls(get(t, 2) + blend(get, t, 3, wide, rows), r, t))
            near = around(rhs, t)
            if t in mids:
                pre[t, pl.ds(SUBS, rows), :] = 9.0 * r + near + 0.5 * first
            gather[t, pl.ds(SUBS, rows), :] = mask[1] * (first + near)
        for t in range(wide):
            other[t, pl.ds(SUBS, rows), :] = seconds[t] + around(gather, t)

    def reflect(q, high):
        turned = pltpu.roll(q, LANES // 2, 1)
        n = q.shape[0]
        at = lax.broadcasted_iota(jnp.int32, (n, LANES), 1) // (2 * edge)
        near, far = (1, 2) if high else (2, 1)
        return jnp.where(at == near, -turned, jnp.where(at == far, -q, 0.0))

    def correct():
        qs = []
        for t in range(wide):
            q = (
                other[t, pl.ds(SUBS, crows, stride=2), :] + other[t, pl.ds(SUBS + 1, crows, stride=2), :]
            )
            qs.append(cmask[spot(t)] * q)
        left, right = mids[0], mids[-1]
        qs[left] = jnp.where(has(has_left), qs[left], reflect(qs[mine[0]], False))
        qs[right] = jnp.where(has(has_right), qs[right], reflect(qs[mine[-1]], True))
        powers = product([qs[t] for t in mids], 2, 4 * LANES, 4 * LANES)
        sides = product(qs, 2, 8 * LANES, 4 * LANES)

        def get(i, k):
            return powers(i - mids[0], k) if k < 4 else sides(i, k - 4)

        b0, b1, b2 = {}, {}, {}
        for t in mids:
            c = get(t, 0)
            j1 = get(t, 1) + blend(get, t, 4, wide, crows)
            j2 = get(t, 2) + blend(get, t, 5, wide, crows)
            j3 = get(t, 3) + (get(t - 1, 7) + get(t + 1, 6))
            coarse[t, pl.ds(SUBS, crows), :] = c
            b0[t] = 729.0 * c + 81.0 * j1 + (9.0 * j2 + j3)
            b1[t] = 81.0 * c + 18.0 * j1 + 3.0 * j2
            b2[t] = 9.0 * c + 3.0 * j1
        for t in mids:
            ea[t, pl.ds(SUBS, crows), :] = cmask[1] * (b2[t] + around(coarse, t, 0, crows))
        for t in mids:
            eb[t, pl.ds(SUBS, crows), :] = cmask[1] * (b1[t] + around(ea, t, 0, crows))
        return {t: b0[t] + around(eb, t, 0, crows) for t in mids}

    scale = CSTEP * STEP * STEP * STEP / 8.0
    square = STEP * STEP

    def finish(e, outs, low, n):
        for t in mids:
            for up in (0, 1):
                gather[t, pl.ds(SUBS + up, crows, stride=2), :] = e[t]
        for t in mids:
            other[t, pl.ds(SUBS + low, n), :] = mask[spot(t), pl.ds(low, n), :] * (
                body(pre, t, low, n) + scale * body(gather, t, low, n)
            )
        get = product([body(other, t, low, n) for t in mids], 3, 0, 4 * LANES)
        first, out = mids[0], {}
        near = len(mids)
        for t in outs:
            i = t - first
            if t in mids:
                value = get(i, 0) + blend(get, i, 1, near, n) + around(other, t, low, n)
            else:
                value = blend(get, i, 1, near, n)
            gather[t, pl.ds(SUBS + low, n), :] = mask[1, pl.ds(low, n), :] * value
        for t in outs:
            i = t - first
            second = blend(get, i, 3, near, n)
            if t in mids:
                second = walls(get(i, 2) + second, body(other, t, low, n), t)
            out[t] = square * (second + around(gather, t, low, n))
            if t in mids:
                out[t] = body(pre, t, low, n) + out[t]
        return out

    def owned(out, low):
        return [own[...] * out[t][edge - low : edge - low + planes] for t in mine]

    def laplace():
        lanes = lax.broadcasted_iota(jnp.int32, (planes, LANES), 1)
        z = lanes % edge
        tile = {t: body(gather, t, edge, planes) for t in mids}
        ahead = {t: pltpu.roll(tile[t], LANES - edge, 1) for t in mids[1:]}
        behind = {t: pltpu.roll(tile[t], edge, 1) for t in mids[:-1]}
        out = []
        for t in mine:
            v = tile[t]
            beside = jnp.where(z < edge - 1, pltpu.roll(v, LANES - 1, 1), 0.0)
            beside = beside + jnp.where(z > 0, pltpu.roll(v, 1, 1), 0.0)
            beside = beside + jnp.where(lanes < LANES - edge, ahead[t], ahead[t + 1])
            beside = beside + jnp.where(lanes >= edge, behind[t], behind[t - 1])
            out.append(square * (own[...] * (6.0 * v - around(gather, t, edge, planes) - beside)))
        return out

    count = count_hbm[0]
    pack(0, source_ref)
    if gossip:
        near = (1 + one(sfc > 0) + one(sfc < n_sfc - 1)) * (1 + one(grp > 0) + one(grp < n_grp - 1))
        pl.semaphore_wait(barrier, near - 1)
    else:
        pl.semaphore_wait(barrier, everyone - 1)
    start(0, source_ref)

    for g, present in enumerate((has_left, 1, has_right)):
        for s in range(slots + 2):
            if s == 0:
                ok = has_below
            else:
                ok = one(count >= s) + one(count == s - 1) * has_above
            value = jnp.full((SUBS, LANES), ok * present, jnp.int32).astype(f32)
            for h in range(edge // SUBS):
                mask[g, pl.ds(s * edge + h * SUBS, SUBS), :] = value
            for h in range(half // SUBS):
                cmask[g, pl.ds(s * half + h * SUBS, SUBS), :] = value
    for s in range(slots):
        value = jnp.full((SUBS, LANES), one(count > s), jnp.int32).astype(f32)
        for h in range(edge // SUBS):
            own[pl.ds(s * edge + h * SUBS, SUBS), :] = value
    pltpu.make_async_copy(weight_ref, weight_ref, local_sem.at[1]).wait()

    settle(1, both)
    tell(0)
    unpack(0, source_ref)
    smooth()
    low, n = SUBS, rows - 2 * SUBS
    out = finish(correct(), mids, low, n)
    for t in mids:
        gather[t, pl.ds(SUBS + low, n), :] = mask[spot(t), pl.ds(low, n), :] * out[t]
    firsts = owned(out, low)
    images = laplace()
    for i, value in enumerate(images):
        image_buf[:, pl.ds(i * LANES, LANES)] = value
    pack(1, image_buf)
    start(1, image_buf)
    hear(0)
    tell(1)
    acc_rz, acc_curv = zero, zero
    for i in range(tiles):
        cols = pl.ds(i * LANES, LANES)
        value = square * firsts[i]
        image = images[i]
        source = body(rhs, mine[i], edge, planes) * own[...]
        first_ref[:, cols] = value
        image_ref[:, cols] = image
        source_out[:, cols] = source
        acc_rz = acc_rz + jnp.sum((source * value).reshape(-1, SUBS, LANES), axis=0)
        acc_curv = acc_curv + jnp.sum((value * image).reshape(-1, SUBS, LANES), axis=0)
    row = lax.broadcasted_iota(jnp.int32, (1, LANES), 1)

    def whole(acc):
        return jnp.sum(jnp.sum(acc, axis=0, keepdims=True), axis=1, keepdims=True)

    rz, curv = whole(acc_rz), whole(acc_curv)
    known = jnp.where(row == 0, rz, jnp.where(row == 1, curv, 0.0))

    for t in range(wide):
        if t in mine:
            rhs[t, pl.ds(SUBS, edge), :] = jnp.zeros((edge, LANES), f32)
            rhs[t, pl.ds(SUBS + edge, planes), :] = images[t - tiles]
            rhs[t, pl.ds(SUBS + edge + planes, edge), :] = jnp.zeros((edge, LANES), f32)
        else:
            rhs[t, pl.ds(SUBS, rows), :] = jnp.zeros((rows, LANES), f32)
    smooth()
    out = finish(correct(), range(wide), 0, rows)
    for t in range(wide):
        dual[t] = mask[spot(t)] * out[t]
    acc = zero
    for t in mine:
        part_of = dual[t, pl.ds(edge, planes), :] * images[t - tiles]
        acc = acc + jnp.sum(part_of.reshape(-1, SUBS, LANES), axis=0)
    settle(2, high)
    pairs = zero
    for g, present in ((1, 1), (2, has_right)):
        for s in range(slots + 2):
            for h in range(edge // SUBS):
                for t in range(tiles):
                    if s == 0:
                        value = jnp.where(has(has_below * present), ghost(below, 1, 1, g, h, t), 0.0)
                    else:
                        value = zero
                        if s >= 2:
                            up = one(count == s - 1) * has_above * present
                            value = jnp.where(has(up), ghost(above, 1, 0, g, h, t), value)
                        if g == 2 and s <= slots:
                            at = pl.ds((s - 1) * edge + h * SUBS, SUBS)
                            centre = side[1, 1, at, pl.ds(t * LANES, LANES)]
                            value = jnp.where(has(one(count >= s) * present), centre, value)
                    if g == 2 or s >= 2:
                        pairs = pairs + dual[g * tiles + t, pl.ds(s * edge + h * SUBS, SUBS), :] * value
    acc = acc + 2.0 * pairs

    def send(slot, device):
        return pltpu.make_async_remote_copy(
            src_ref=part, dst_ref=red.at[slot], send_sem=red_sem.at[0],
            recv_sem=red_sem.at[1], device_id=device, device_id_type=MESH,
        )

    value = jnp.concatenate([square * jnp.sum(acc, axis=0, keepdims=True), known], axis=0)
    part[...] = value
    red[me] = value
    hear(1)

    if everyone <= 64:
        turn = jnp.where(2 * sfc >= n_sfc, 1, n_sfc - 1)
        grps = [lax.rem(grp + i, n_grp) for i in range(n_grp)]
        for ds in (*range(1, n_sfc), 0):
            there_sfc = lax.rem(sfc + ds * turn, n_sfc)
            for dg in range(n_grp):
                if ds or dg:
                    send(me, {"sfc": there_sfc, "grp": grps[dg]}).start()
    else:
        def go(i, carry):
            peer, device = place(i)
            send(me, device).start()
            return carry

        lax.fori_loop(1, everyone, go, 0)
    settle(3, low_end)
    unpack(1, image_buf)
    smooth()
    for i, value in enumerate(owned(finish(correct(), mine, SUBS, rows - 2 * SUBS), SUBS)):
        w_ref[:, pl.ds(i * LANES, LANES)] = square * value
    settle(0, both, 2)

    rest = red.at[pl.ds(0, everyone - 1)]
    pltpu.make_async_copy(rest, rest, red_sem.at[0]).wait()
    pltpu.make_async_copy(rest, rest, red_sem.at[1]).wait()
    sums = jnp.sum(red[...], axis=0)

    def pick(value):
        return jnp.sum(value, axis=1, keepdims=True)

    rz = pick(jnp.where(row == 0, sums[1:], 0.0))
    inverse = 1.0 / pick(jnp.where(row == 1, sums[1:], 0.0))
    alpha = rz * inverse
    ratio = pick(sums[:1]) * inverse
    scale_ref[...] = jnp.concatenate(
        [jnp.broadcast_to(alpha, (1, LANES)), jnp.broadcast_to(ratio, (1, LANES))], axis=0
    )


def combine(first, image, w, source, scale, solution_ref, residual_ref, direction_ref):
    alpha = scale[0:1, 0:1]
    ratio = scale[1:2, 0:1]
    solution_ref[...] = alpha * first[...]
    residual_ref[...] = source[...] - alpha * image[...]
    direction_ref[...] = alpha * (ratio * first[...] - w[...])


def shards(n_sfc, n_grp, source, layer_counts):
    slots, edge, width = source.shape
    planes, tiles = slots * edge, width // LANES
    rows, crows = (slots + 2) * edge, (slots + 2) * edge // 2
    f32 = jnp.float32
    vmem = pltpu.VMEM
    dma = pltpu.SemaphoreType.DMA
    n = n_sfc * n_grp
    out = jax.ShapeDtypeStruct((planes, width), f32)
    fine = vmem((3 * tiles, rows + 2 * SUBS, LANES), f32)
    coarse = vmem((3 * tiles, crows + 2 * SUBS, LANES), f32)
    parts = pl.pallas_call(
        functools.partial(kernel, (slots, edge, tiles, n_sfc, n_grp)),
        out_shape=(out, out, out, out, jax.ShapeDtypeStruct((2, LANES), f32)),
        in_specs=[pl.BlockSpec(memory_space=pltpu.SMEM)] + [pl.BlockSpec(memory_space=pltpu.HBM)] * 2,
        out_specs=[pl.BlockSpec(memory_space=pltpu.VMEM)] * 5,
        scratch_shapes=[
            vmem((planes, width), f32),
            vmem((planes, width), f32),
            vmem((3 * LANES, 12 * LANES), jnp.bfloat16),
            fine, fine, fine, fine,
            vmem((3 * tiles, rows, LANES), f32),
            coarse, coarse, coarse,
            vmem((3, rows, LANES), f32),
            vmem((3, crows, LANES), f32),
            vmem((planes, LANES), f32),
            vmem((2, 2, 5, SUBS, LANES), f32),
            vmem((2, 2, planes, width), f32),
            vmem((2, 3, 3, SUBS, LANES), f32),
            vmem((2, 3, 3, SUBS, LANES), f32),
            vmem((2, LANES), f32),
            vmem((n, 2, LANES), f32),
            vmem((4 * planes * tiles // SUBS + 28, SUBS, LANES), f32),
            dma((2,)),
            dma((4,)),
            dma((2,)),
            pltpu.SemaphoreType.REGULAR((2,)),
        ],
        compiler_params=pltpu.CompilerParams(
            collective_id=0, has_side_effects=True, vmem_limit_bytes=16 * 1024 * 1024
        ),
        name="pcg",
    )(layer_counts, pltpu.with_memory_space_constraint(source.reshape(planes, width), pltpu.HBM), pltpu.with_memory_space_constraint(jnp.asarray(weights(edge)), pltpu.HBM))
    outs = pl.pallas_call(
        combine,
        out_shape=(out, out, out),
        in_specs=[pl.BlockSpec(memory_space=pltpu.VMEM)] * 5,
        out_specs=[pl.BlockSpec(memory_space=pltpu.VMEM)] * 3,
        compiler_params=pltpu.CompilerParams(vmem_limit_bytes=16 * 1024 * 1024),
        name="combine",
    )(*parts)
    return tuple(o.reshape(source.shape) for o in outs)


def solution(mesh):
    n_sfc, n_grp = mesh.shape["sfc"], mesh.shape["grp"]
    return jax.shard_map(
        functools.partial(shards, n_sfc, n_grp),
        mesh=mesh,
        in_specs=(P("sfc", None, "grp"), P("sfc")),
        out_specs=(P("sfc", None, "grp"), P("sfc", None, "grp"), P("sfc", None, "grp")),
        check_vma=False,
    )
```

```python
import functools

import jax
import jax.numpy as jnp
import numpy as np
from jax import lax
from jax.experimental import pallas as pl
from jax.experimental.pallas import tpu as pltpu
from jax.sharding import PartitionSpec as P

MESH = pl.DeviceIdType.MESH
LANES = 128
SUBS = 8
STEP = 1.0 / 9.0
CSTEP = 4.0 / 9.0
WAYS = ((1, 1), (1, -1), (-1, 1), (-1, -1), (1, 0), (-1, 0), (0, 1), (0, -1))


def weights(edge):
    lane = np.arange(LANES)
    y, z = lane // edge, lane % edge

    def parts(y, z, last):
        dy, dz = y[None, :] - y[:, None], z[None, :] - z[:, None]
        one = 3.0 * ((dy == 0) & (dz == 0)) + ((dy == 0) & (abs(dz) == 1)) + ((abs(dy) == 1) & (dz == 0))
        down = 1.0 * ((dy == last) & (dz == 0))
        up = 1.0 * ((dy == -last) & (dz == 0))
        return one, down, up

    one, down, up = parts(y, z, SUBS - 1)
    two = one @ one + down @ up + up @ down
    side = down + up
    fine = [2 * one, 2 * side, two, one @ side + side @ one]
    one, down, up = parts(y // 2, z // 2, SUBS // 2 - 1)
    same = 1.0 * ((y[None, :] // 2 == y[:, None] // 2) & (z[None, :] // 2 == z[:, None] // 2))
    two = (one @ one + down @ up + up @ down) / 4
    down2, up2 = (one @ down + down @ one) / 4, (one @ up + up @ one) / 4
    three = (two @ one + down2 @ up + up2 @ down) / 4
    down3, up3 = (two @ down + down2 @ one) / 4, (two @ up + up2 @ one) / 4
    coarse = [same, one, two, three, down + up, down2 + up2, down3, up3]
    whole = np.concatenate(fine + coarse, axis=1)
    return whole.astype(jnp.bfloat16)


def split(x, pieces):
    out = []
    for i in range(pieces):
        part = x.astype(jnp.bfloat16)
        out.append(part)
        if i < pieces - 1:
            x = x - part.astype(jnp.float32)
    return out


def kernel(
    dims, count_hbm, source_hbm, weight_hbm, first_ref, image_ref, w_ref, source_out, scale_ref,
    source_ref, image_buf, weight_ref, rhs, pre, gather, other, dual, coarse, ea, eb,
    mask, cmask, own, packed, side, below, above, part, red, dummy, local_sem,
    trade_sem, red_sem, hello,
):
    slots, edge, tiles, n_sfc, n_grp = dims
    half = edge // 2
    planes = slots * edge
    rows, crows = (slots + 2) * edge, (slots + 2) * half
    wide = 3 * tiles
    mids = tuple(range(tiles - 1, 2 * tiles + 1))
    mine = tuple(range(tiles, 2 * tiles))
    f32 = jnp.float32
    sfc = lax.axis_index("sfc")
    grp = lax.axis_index("grp")
    me = sfc * n_grp + grp
    everyone = n_sfc * n_grp

    def there(ds, dg):
        flag = None
        if ds:
            flag = sfc < n_sfc - 1 if ds > 0 else sfc > 0
        if dg:
            extra = grp < n_grp - 1 if dg > 0 else grp > 0
            flag = extra if flag is None else jnp.logical_and(flag, extra)
        return flag

    gossip = n_sfc <= 9 and n_grp <= 4
    barrier = pltpu.get_barrier_semaphore()

    def place(i):
        peer = lax.rem(me + i, everyone)
        return peer, {"sfc": peer // n_grp, "grp": lax.rem(peer, n_grp)}

    def greet(i, carry):
        pl.semaphore_signal(barrier, inc=1, device_id=place(i)[1], device_id_type=MESH)
        return carry

    if gossip:
        for ds, dg in WAYS:
            @pl.when(there(ds, dg))
            def _(ds=ds, dg=dg):
                pl.semaphore_signal(
                    barrier, inc=1, device_id={"sfc": sfc + ds, "grp": grp + dg},
                    device_id_type=MESH,
                )
    else:
        lax.fori_loop(1, everyone, greet, 0)

    source_copy = pltpu.make_async_copy(source_hbm, source_ref, local_sem.at[0])
    source_copy.start()
    for up in range(3):
        pltpu.make_async_copy(
            weight_hbm, weight_ref.at[pl.ds(up * LANES, LANES), :], local_sem.at[1]
        ).start()
    def one(flag):
        return jnp.where(flag, 1, 0)

    rounds = (((2, 1), (2, -1), (-2, 1), (-2, -1), (0, 1), (0, -1)), ((4, 0), (-4, 0)))

    def inside(ds, dg):
        flag = sfc + ds < n_sfc if ds >= 0 else sfc + ds >= 0
        return jnp.logical_and(flag, grp + dg < n_grp if dg >= 0 else grp + dg >= 0)

    def tell(rnd):
        if gossip:
            for ds, dg in rounds[rnd]:
                @pl.when(inside(ds, dg))
                def _(ds=ds, dg=dg):
                    pl.semaphore_signal(
                        hello.at[rnd], inc=1, device_id={"sfc": sfc + ds, "grp": grp + dg},
                        device_id_type=MESH,
                    )

    def hear(rnd):
        if gossip:
            pl.semaphore_wait(hello.at[rnd], sum(one(inside(ds, dg)) for ds, dg in rounds[rnd]))

    lane = lax.broadcasted_iota(jnp.int32, (SUBS, LANES), 1)
    low_half = lane < LANES // 2

    def has(flag_int):
        return flag_int > 0

    has_below = one(sfc > 0)
    has_above = one(sfc < n_sfc - 1)
    has_left = one(grp > 0)
    has_right = one(grp < n_grp - 1)

    zero = jnp.zeros((SUBS, LANES), f32)
    for ref in (rhs, pre, gather, other):
        for t in range(wide):
            ref[t, pl.ds(0, SUBS), :] = zero
            ref[t, pl.ds(SUBS + rows, SUBS), :] = zero
    for t in range(wide):
        for ref in (coarse, ea, eb):
            ref[t, pl.ds(0, SUBS), :] = zero
            ref[t, pl.ds(SUBS + crows, SUBS), :] = zero
    for t in range(wide):
        for at in (SUBS, rows):
            other[t, pl.ds(at, SUBS), :] = zero

    source_copy.wait()

    def copies(e, ds, dg, src):
        gpos = 1 - dg
        if ds == 0:
            source, target = src, side.at[e, gpos // 2]
        else:
            tile, amount = ((0, 2), (1, 3), (3, 2))[dg + 1]
            source = packed.at[e, int(ds > 0), pl.ds(tile, amount)]
            target = (below if ds > 0 else above).at[e, gpos, pl.ds(0, amount)]
        return pltpu.make_async_remote_copy(
            src_ref=source, dst_ref=target, send_sem=trade_sem.at[0],
            recv_sem=trade_sem.at[1 if e == 0 else 2 if (dg, ds) < (0, 0) else 3], device_id={"sfc": sfc + ds, "grp": grp + dg},
            device_id_type=MESH,
        )

    def start(e, src):
        for ds, dg in WAYS:
            @pl.when(there(ds, dg))
            def _(ds=ds, dg=dg):
                copies(e, ds, dg, src).start()

    column = slots * edge * tiles // SUBS
    ends, layers = has_left + has_right, has_below + has_above

    def settle(sem, amounts, times=1):
        for flags, tiles_in in amounts:
            if tiles_in:
                @pl.when(functools.reduce(jnp.logical_and, flags))
                def _(tiles_in=tiles_in):
                    ref = dummy.at[pl.ds(0, times * tiles_in)]
                    pltpu.make_async_copy(ref, ref, trade_sem.at[sem]).wait()

    def half_of(beside, along):
        return [
            ((beside == b, along == a, layers == l), b * (column + 2 * l) + 3 * a)
            for b in (0, 1) for l in (0, 1, 2) for a in (0, 1) if l - 1 <= a <= l
        ]

    both = [((ends == b, layers == l), b * (column + 2 * l) + 3 * l) for b in range(3) for l in range(3)]
    high, low_end = half_of(has_right, has_above), half_of(has_left, has_below)

    def pack(e, src):
        cut = SUBS // 2
        for up in (0, 1):
            at = pl.ds(0, edge)
            value = [src[at, pl.ds(t * LANES, LANES)] for t in range(tiles)]
            if up:
                for s in range(1, slots):
                    at = pl.ds(s * edge, edge)
                    value = [
                        jnp.where(count > s, src[at, pl.ds(t * LANES, LANES)], value[t])
                        for t in range(tiles)
                    ]
            if up:
                near = [v[edge - SUBS :] for v in value]
                far = [v[edge - SUBS - cut : edge - SUBS] for v in value]
                edges = [v[edge - cut :] for v in value]
            else:
                near = [v[:SUBS] for v in value]
                far = [v[SUBS : SUBS + cut] for v in value]
                edges = [v[:cut] for v in value]
            packed[e, up, 0] = jnp.concatenate([far[0], edges[1]], axis=0)
            packed[e, up, 1] = near[0]
            packed[e, up, 2] = jnp.concatenate([far[0], far[1]], axis=0)
            packed[e, up, 3] = near[1]
            packed[e, up, 4] = jnp.concatenate([far[1], edges[0]], axis=0)

    def ghost(ref, e, up, g, h, t):
        cut = SUBS // 2
        near_h = 1 if up else 0
        if g == 1:
            if h == near_h:
                return ref[e, g, 0 if t == 0 else 2]
            mix, low = ref[e, g, 1], t == 0
        else:
            full = 1 if g == 0 else 0
            if h == near_h and t == full:
                return ref[e, g, 0 if g == 0 else 1]
            mix = ref[e, g, 1 if g == 0 else 0]
            if h == near_h:
                low = False
            elif t == full:
                low = True
            else:
                return jnp.zeros((SUBS, LANES), f32)
        part = mix[:cut] if low else mix[cut:]
        none = jnp.zeros((cut, LANES), f32)
        return jnp.concatenate([none, part] if up else [part, none], axis=0)

    def unpack(e, src):
        sides = ((0, has_left), (1, 1), (2, has_right))
        for g, present in sides:
            for s in range(slots + 2):
                for h in range(edge // SUBS):
                    for t in range(tiles):
                        cols = pl.ds(t * LANES, LANES)

                        def centre(slot):
                            at = pl.ds(slot * edge + h * SUBS, SUBS)
                            return src[at, cols] if g == 1 else side[e, g // 2, at, cols]

                        if s == 0:
                            value = jnp.where(has(has_below * present), ghost(below, e, 1, g, h, t), 0.0)
                        else:
                            up = one(count == s - 1) * has_above * present
                            value = jnp.zeros((SUBS, LANES), f32)
                            if s >= 2:
                                value = jnp.where(has(up), ghost(above, e, 0, g, h, t), value)
                            if s <= slots:
                                value = jnp.where(has(one(count >= s) * present), centre(s - 1), value)
                        rhs[g * tiles + t, pl.ds(SUBS + s * edge + h * SUBS, SUBS), :] = value

    def body(ref, t, first=0, n=rows):
        return ref[t, pl.ds(SUBS + first, n), :]

    def around(ref, t, first=0, n=rows):
        return ref[t, pl.ds(SUBS + first - 1, n), :] + ref[t, pl.ds(SUBS + first + 1, n), :]

    def spot(t):
        return t // tiles

    def product(values, pieces, at, width):
        n = values[0].shape[0]
        parts = [split(v, pieces) for v in values]
        lhs = jnp.concatenate([jnp.concatenate(p, axis=1) for p in parts], axis=0)
        w = weight_ref[pl.ds(0, pieces * LANES), pl.ds(at, width)]
        out = jnp.dot(lhs, w, preferred_element_type=f32)

        def get(i, k):
            return out[i * n : (i + 1) * n, k * LANES : (k + 1) * LANES]

        return get

    def halves(n):
        return jnp.broadcast_to(low_half[:1], (n, LANES))

    def cross(get, i, k, k_up, count_, n):
        none = jnp.zeros((n, LANES), f32)
        lower = get(i - 1, k_up) if 0 < i <= count_ else none
        upper = get(i + 1, k) if -1 <= i < count_ - 1 else none
        return lower, upper

    def blend(get, i, k, amount, n):
        lower, upper = cross(get, i, k, k, amount, n)
        return jnp.where(halves(n), lower, upper)

    low_wall = jnp.where(jnp.logical_and(lane < edge, grp == 0), 1.0, 0.0)
    high_wall = jnp.where(jnp.logical_and(lane >= LANES - edge, grp == n_grp - 1), 1.0, 0.0)

    def walls(value, x, t):
        n = value.shape[0]
        if t == mine[0]:
            value = value - x * jnp.broadcast_to(low_wall[:1], (n, LANES))
        if t == mine[-1]:
            value = value - x * jnp.broadcast_to(high_wall[:1], (n, LANES))
        return value

    def smooth():
        get = product([body(rhs, t) for t in range(wide)], 2, 0, 4 * LANES)
        seconds = []
        for t in range(wide):
            r = body(rhs, t)
            first = get(t, 0) + blend(get, t, 1, wide, rows)
            seconds.append(walls(get(t, 2) + blend(get, t, 3, wide, rows), r, t))
            near = around(rhs, t)
            if t in mids:
                pre[t, pl.ds(SUBS, rows), :] = 9.0 * r + near + 0.5 * first
            gather[t, pl.ds(SUBS, rows), :] = mask[1] * (first + near)
        for t in range(wide):
            other[t, pl.ds(SUBS, rows), :] = seconds[t] + around(gather, t)

    def reflect(q, high):
        turned = pltpu.roll(q, LANES // 2, 1)
        n = q.shape[0]
        at = lax.broadcasted_iota(jnp.int32, (n, LANES), 1) // (2 * edge)
        near, far = (1, 2) if high else (2, 1)
        return jnp.where(at == near, -turned, jnp.where(at == far, -q, 0.0))

    def correct():
        qs = []
        for t in range(wide):
            q = (
                other[t, pl.ds(SUBS, crows, stride=2), :] + other[t, pl.ds(SUBS + 1, crows, stride=2), :]
            )
            qs.append(cmask[spot(t)] * q)
        left, right = mids[0], mids[-1]
        qs[left] = jnp.where(has(has_left), qs[left], reflect(qs[mine[0]], False))
        qs[right] = jnp.where(has(has_right), qs[right], reflect(qs[mine[-1]], True))
        powers = product([qs[t] for t in mids], 2, 4 * LANES, 4 * LANES)
        sides = product(qs, 2, 8 * LANES, 4 * LANES)

        def get(i, k):
            return powers(i - mids[0], k) if k < 4 else sides(i, k - 4)

        b0, b1, b2 = {}, {}, {}
        for t in mids:
            c = get(t, 0)
            j1 = get(t, 1) + blend(get, t, 4, wide, crows)
            j2 = get(t, 2) + blend(get, t, 5, wide, crows)
            j3 = get(t, 3) + (get(t - 1, 7) + get(t + 1, 6))
            coarse[t, pl.ds(SUBS, crows), :] = c
            b0[t] = 729.0 * c + 81.0 * j1 + (9.0 * j2 + j3)
            b1[t] = 81.0 * c + 18.0 * j1 + 3.0 * j2
            b2[t] = 9.0 * c + 3.0 * j1
        for t in mids:
            ea[t, pl.ds(SUBS, crows), :] = cmask[1] * (b2[t] + around(coarse, t, 0, crows))
        for t in mids:
            eb[t, pl.ds(SUBS, crows), :] = cmask[1] * (b1[t] + around(ea, t, 0, crows))
        return {t: b0[t] + around(eb, t, 0, crows) for t in mids}

    scale = CSTEP * STEP * STEP * STEP / 8.0
    square = STEP * STEP

    def finish(e, outs, low, n):
        for t in mids:
            for up in (0, 1):
                gather[t, pl.ds(SUBS + up, crows, stride=2), :] = e[t]
        for t in mids:
            other[t, pl.ds(SUBS + low, n), :] = mask[spot(t), pl.ds(low, n), :] * (
                body(pre, t, low, n) + scale * body(gather, t, low, n)
            )
        get = product([body(other, t, low, n) for t in mids], 3, 0, 4 * LANES)
        first, out = mids[0], {}
        near = len(mids)
        for t in outs:
            i = t - first
            if t in mids:
                value = get(i, 0) + blend(get, i, 1, near, n) + around(other, t, low, n)
            else:
                value = blend(get, i, 1, near, n)
            gather[t, pl.ds(SUBS + low, n), :] = mask[1, pl.ds(low, n), :] * value
        for t in outs:
            i = t - first
            second = blend(get, i, 3, near, n)
            if t in mids:
                second = walls(get(i, 2) + second, body(other, t, low, n), t)
            out[t] = square * (second + around(gather, t, low, n))
            if t in mids:
                out[t] = body(pre, t, low, n) + out[t]
        return out

    def owned(out, low):
        return [own[...] * out[t][edge - low : edge - low + planes] for t in mine]

    def laplace():
        lanes = lax.broadcasted_iota(jnp.int32, (planes, LANES), 1)
        z = lanes % edge
        tile = {t: body(gather, t, edge, planes) for t in mids}
        ahead = {t: pltpu.roll(tile[t], LANES - edge, 1) for t in mids[1:]}
        behind = {t: pltpu.roll(tile[t], edge, 1) for t in mids[:-1]}
        out = []
        for t in mine:
            v = tile[t]
            beside = jnp.where(z < edge - 1, pltpu.roll(v, LANES - 1, 1), 0.0)
            beside = beside + jnp.where(z > 0, pltpu.roll(v, 1, 1), 0.0)
            beside = beside + jnp.where(lanes < LANES - edge, ahead[t], ahead[t + 1])
            beside = beside + jnp.where(lanes >= edge, behind[t], behind[t - 1])
            out.append(square * (own[...] * (6.0 * v - around(gather, t, edge, planes) - beside)))
        return out

    count = count_hbm[0]
    pack(0, source_ref)
    if gossip:
        near = (1 + one(sfc > 0) + one(sfc < n_sfc - 1)) * (1 + one(grp > 0) + one(grp < n_grp - 1))
        pl.semaphore_wait(barrier, near - 1)
    else:
        pl.semaphore_wait(barrier, everyone - 1)
    start(0, source_ref)

    for g, present in enumerate((has_left, 1, has_right)):
        for s in range(slots + 2):
            if s == 0:
                ok = has_below
            else:
                ok = one(count >= s) + one(count == s - 1) * has_above
            value = jnp.full((SUBS, LANES), ok * present, jnp.int32).astype(f32)
            for h in range(edge // SUBS):
                mask[g, pl.ds(s * edge + h * SUBS, SUBS), :] = value
            for h in range(half // SUBS):
                cmask[g, pl.ds(s * half + h * SUBS, SUBS), :] = value
    for s in range(slots):
        value = jnp.full((SUBS, LANES), one(count > s), jnp.int32).astype(f32)
        for h in range(edge // SUBS):
            own[pl.ds(s * edge + h * SUBS, SUBS), :] = value
    pltpu.make_async_copy(weight_ref, weight_ref, local_sem.at[1]).wait()

    settle(1, both)
    tell(0)
    unpack(0, source_ref)
    smooth()
    low, n = SUBS, rows - 2 * SUBS
    out = finish(correct(), mids, low, n)
    for t in mids:
        gather[t, pl.ds(SUBS + low, n), :] = mask[spot(t), pl.ds(low, n), :] * out[t]
    firsts = owned(out, low)
    images = laplace()
    for i, value in enumerate(images):
        image_buf[:, pl.ds(i * LANES, LANES)] = value
    pack(1, image_buf)
    start(1, image_buf)
    hear(0)
    tell(1)
    acc_rz, acc_curv = zero, zero
    for i in range(tiles):
        cols = pl.ds(i * LANES, LANES)
        value = square * firsts[i]
        image = images[i]
        source = body(rhs, mine[i], edge, planes) * own[...]
        first_ref[:, cols] = value
        image_ref[:, cols] = image
        source_out[:, cols] = source
        acc_rz = acc_rz + jnp.sum((source * value).reshape(-1, SUBS, LANES), axis=0)
        acc_curv = acc_curv + jnp.sum((value * image).reshape(-1, SUBS, LANES), axis=0)
    row = lax.broadcasted_iota(jnp.int32, (1, LANES), 1)

    def whole(acc):
        return jnp.sum(jnp.sum(acc, axis=0, keepdims=True), axis=1, keepdims=True)

    rz, curv = whole(acc_rz), whole(acc_curv)
    known = jnp.where(row == 0, rz, jnp.where(row == 1, curv, 0.0))

    for t in range(wide):
        if t in mine:
            rhs[t, pl.ds(SUBS, edge), :] = jnp.zeros((edge, LANES), f32)
            rhs[t, pl.ds(SUBS + edge, planes), :] = images[t - tiles]
            rhs[t, pl.ds(SUBS + edge + planes, edge), :] = jnp.zeros((edge, LANES), f32)
        else:
            rhs[t, pl.ds(SUBS, rows), :] = jnp.zeros((rows, LANES), f32)
    smooth()
    out = finish(correct(), range(wide), 0, rows)
    for t in range(wide):
        dual[t] = mask[spot(t)] * out[t]
    acc = zero
    for t in mine:
        part_of = dual[t, pl.ds(edge, planes), :] * images[t - tiles]
        acc = acc + jnp.sum(part_of.reshape(-1, SUBS, LANES), axis=0)
    settle(2, high)
    pairs = zero
    for g, present in ((1, 1), (2, has_right)):
        for s in range(slots + 2):
            for h in range(edge // SUBS):
                for t in range(tiles):
                    if s == 0:
                        value = jnp.where(has(has_below * present), ghost(below, 1, 1, g, h, t), 0.0)
                    else:
                        value = zero
                        if s >= 2:
                            up = one(count == s - 1) * has_above * present
                            value = jnp.where(has(up), ghost(above, 1, 0, g, h, t), value)
                        if g == 2 and s <= slots:
                            at = pl.ds((s - 1) * edge + h * SUBS, SUBS)
                            centre = side[1, 1, at, pl.ds(t * LANES, LANES)]
                            value = jnp.where(has(one(count >= s) * present), centre, value)
                    if g == 2 or s >= 2:
                        pairs = pairs + dual[g * tiles + t, pl.ds(s * edge + h * SUBS, SUBS), :] * value
    acc = acc + 2.0 * pairs

    def send(slot, device):
        return pltpu.make_async_remote_copy(
            src_ref=part, dst_ref=red.at[slot], send_sem=red_sem.at[0],
            recv_sem=red_sem.at[1], device_id=device, device_id_type=MESH,
        )

    value = jnp.concatenate([square * jnp.sum(acc, axis=0, keepdims=True), known], axis=0)
    part[...] = value
    red[me] = value
    hear(1)

    if everyone <= 64:
        for i in range(n_sfc - 1):
            other_sfc = i + one(i >= sfc)
            for g in range(n_grp):
                send(me, {"sfc": other_sfc, "grp": g}).start()
        for i in range(n_grp - 1):
            send(me, {"sfc": sfc, "grp": i + one(i >= grp)}).start()
    else:
        def go(i, carry):
            peer, device = place(i)
            send(me, device).start()
            return carry

        lax.fori_loop(1, everyone, go, 0)
    settle(3, low_end)
    unpack(1, image_buf)
    smooth()
    for i, value in enumerate(owned(finish(correct(), mine, SUBS, rows - 2 * SUBS), SUBS)):
        w_ref[:, pl.ds(i * LANES, LANES)] = square * value
    settle(0, both, 2)

    rest = red.at[pl.ds(0, everyone - 1)]
    pltpu.make_async_copy(rest, rest, red_sem.at[0]).wait()
    pltpu.make_async_copy(rest, rest, red_sem.at[1]).wait()
    sums = red[...]
    while sums.shape[0] % 2 == 0:
        sums = sums[: sums.shape[0] // 2] + sums[sums.shape[0] // 2 :]
    sums = jnp.sum(sums, axis=0)

    def pick(value):
        return jnp.sum(value, axis=1, keepdims=True)

    rz = pick(jnp.where(row == 0, sums[1:], 0.0))
    inverse = 1.0 / pick(jnp.where(row == 1, sums[1:], 0.0))
    alpha = rz * inverse
    ratio = pick(sums[:1]) * inverse
    scale_ref[...] = jnp.concatenate(
        [jnp.broadcast_to(alpha, (1, LANES)), jnp.broadcast_to(ratio, (1, LANES))], axis=0
    )


def combine(first, image, w, source, scale, solution_ref, residual_ref, direction_ref):
    alpha = scale[0:1, 0:1]
    ratio = scale[1:2, 0:1]
    solution_ref[...] = alpha * first[...]
    residual_ref[...] = source[...] - alpha * image[...]
    direction_ref[...] = alpha * (ratio * first[...] - w[...])


def shards(n_sfc, n_grp, source, layer_counts):
    slots, edge, width = source.shape
    planes, tiles = slots * edge, width // LANES
    rows, crows = (slots + 2) * edge, (slots + 2) * edge // 2
    f32 = jnp.float32
    vmem = pltpu.VMEM
    dma = pltpu.SemaphoreType.DMA
    n = n_sfc * n_grp
    out = jax.ShapeDtypeStruct((planes, width), f32)
    fine = vmem((3 * tiles, rows + 2 * SUBS, LANES), f32)
    coarse = vmem((3 * tiles, crows + 2 * SUBS, LANES), f32)
    parts = pl.pallas_call(
        functools.partial(kernel, (slots, edge, tiles, n_sfc, n_grp)),
        out_shape=(out, out, out, out, jax.ShapeDtypeStruct((2, LANES), f32)),
        in_specs=[pl.BlockSpec(memory_space=pltpu.SMEM)] + [pl.BlockSpec(memory_space=pltpu.HBM)] * 2,
        out_specs=[pl.BlockSpec(memory_space=pltpu.VMEM)] * 5,
        scratch_shapes=[
            vmem((planes, width), f32),
            vmem((planes, width), f32),
            vmem((3 * LANES, 12 * LANES), jnp.bfloat16),
            fine, fine, fine, fine,
            vmem((3 * tiles, rows, LANES), f32),
            coarse, coarse, coarse,
            vmem((3, rows, LANES), f32),
            vmem((3, crows, LANES), f32),
            vmem((planes, LANES), f32),
            vmem((2, 2, 5, SUBS, LANES), f32),
            vmem((2, 2, planes, width), f32),
            vmem((2, 3, 3, SUBS, LANES), f32),
            vmem((2, 3, 3, SUBS, LANES), f32),
            vmem((2, LANES), f32),
            vmem((n, 2, LANES), f32),
            vmem((4 * planes * tiles // SUBS + 28, SUBS, LANES), f32),
            dma((2,)),
            dma((4,)),
            dma((2,)),
            pltpu.SemaphoreType.REGULAR((2,)),
        ],
        compiler_params=pltpu.CompilerParams(
            collective_id=0, has_side_effects=True, vmem_limit_bytes=16 * 1024 * 1024
        ),
        name="pcg",
    )(layer_counts, pltpu.with_memory_space_constraint(source.reshape(planes, width), pltpu.HBM), pltpu.with_memory_space_constraint(jnp.asarray(weights(edge)), pltpu.HBM))
    outs = pl.pallas_call(
        combine,
        out_shape=(out, out, out),
        in_specs=[pl.BlockSpec(memory_space=pltpu.VMEM)] * 5,
        out_specs=[pl.BlockSpec(memory_space=pltpu.VMEM)] * 3,
        compiler_params=pltpu.CompilerParams(vmem_limit_bytes=16 * 1024 * 1024),
        name="combine",
    )(*parts)
    return tuple(o.reshape(source.shape) for o in outs)


def solution(mesh):
    n_sfc, n_grp = mesh.shape["sfc"], mesh.shape["grp"]
    return jax.shard_map(
        functools.partial(shards, n_sfc, n_grp),
        mesh=mesh,
        in_specs=(P("sfc", None, "grp"), P("sfc")),
        out_specs=(P("sfc", None, "grp"), P("sfc", None, "grp"), P("sfc", None, "grp")),
        check_vma=False,
    )
```

```python
import functools

import jax
import jax.numpy as jnp
import numpy as np
from jax import lax
from jax.experimental import pallas as pl
from jax.experimental.pallas import tpu as pltpu
from jax.sharding import PartitionSpec as P

MESH = pl.DeviceIdType.MESH
LANES = 128
SUBS = 8
STEP = 1.0 / 9.0
CSTEP = 4.0 / 9.0
WAYS = ((1, 1), (1, -1), (-1, 1), (-1, -1), (1, 0), (-1, 0), (0, 1), (0, -1))


def weights(edge):
    lane = np.arange(LANES)
    y, z = lane // edge, lane % edge

    def parts(y, z, last):
        dy, dz = y[None, :] - y[:, None], z[None, :] - z[:, None]
        one = 3.0 * ((dy == 0) & (dz == 0)) + ((dy == 0) & (abs(dz) == 1)) + ((abs(dy) == 1) & (dz == 0))
        down = 1.0 * ((dy == last) & (dz == 0))
        up = 1.0 * ((dy == -last) & (dz == 0))
        return one, down, up

    one, down, up = parts(y, z, SUBS - 1)
    two = one @ one + down @ up + up @ down
    side = down + up
    fine = [2 * one, 2 * side, two, one @ side + side @ one]
    one, down, up = parts(y // 2, z // 2, SUBS // 2 - 1)
    same = 1.0 * ((y[None, :] // 2 == y[:, None] // 2) & (z[None, :] // 2 == z[:, None] // 2))
    two = (one @ one + down @ up + up @ down) / 4
    down2, up2 = (one @ down + down @ one) / 4, (one @ up + up @ one) / 4
    three = (two @ one + down2 @ up + up2 @ down) / 4
    down3, up3 = (two @ down + down2 @ one) / 4, (two @ up + up2 @ one) / 4
    coarse = [same, one, two, three, down + up, down2 + up2, down3, up3]
    whole = np.concatenate(fine + coarse, axis=1)
    return whole.astype(jnp.bfloat16)


def split(x, pieces):
    out = []
    for i in range(pieces):
        part = x.astype(jnp.bfloat16)
        out.append(part)
        if i < pieces - 1:
            x = x - part.astype(jnp.float32)
    return out


def kernel(
    dims, count_hbm, source_hbm, weight_hbm, first_ref, image_ref, w_ref, source_out, scale_ref,
    source_ref, image_buf, weight_ref, rhs, pre, gather, other, dual, coarse, ea, eb,
    mask, cmask, own, packed, side, below, above, part, red, dummy, local_sem,
    trade_sem, red_sem, hello,
):
    slots, edge, tiles, n_sfc, n_grp = dims
    half = edge // 2
    planes = slots * edge
    rows, crows = (slots + 2) * edge, (slots + 2) * half
    wide = 3 * tiles
    mids = tuple(range(tiles - 1, 2 * tiles + 1))
    mine = tuple(range(tiles, 2 * tiles))
    f32 = jnp.float32
    sfc = lax.axis_index("sfc")
    grp = lax.axis_index("grp")
    me = sfc * n_grp + grp
    everyone = n_sfc * n_grp

    def there(ds, dg):
        flag = None
        if ds:
            flag = sfc < n_sfc - 1 if ds > 0 else sfc > 0
        if dg:
            extra = grp < n_grp - 1 if dg > 0 else grp > 0
            flag = extra if flag is None else jnp.logical_and(flag, extra)
        return flag

    gossip = n_sfc <= 9 and n_grp <= 4
    barrier = pltpu.get_barrier_semaphore()

    def place(i):
        peer = lax.rem(me + i, everyone)
        return peer, {"sfc": peer // n_grp, "grp": lax.rem(peer, n_grp)}

    def greet(i, carry):
        pl.semaphore_signal(barrier, inc=1, device_id=place(i)[1], device_id_type=MESH)
        return carry

    if gossip:
        for ds, dg in WAYS:
            @pl.when(there(ds, dg))
            def _(ds=ds, dg=dg):
                pl.semaphore_signal(
                    barrier, inc=1, device_id={"sfc": sfc + ds, "grp": grp + dg},
                    device_id_type=MESH,
                )
    else:
        lax.fori_loop(1, everyone, greet, 0)

    source_copy = pltpu.make_async_copy(source_hbm, source_ref, local_sem.at[0])
    source_copy.start()
    for up in range(3):
        pltpu.make_async_copy(
            weight_hbm, weight_ref.at[pl.ds(up * LANES, LANES), :], local_sem.at[1]
        ).start()
    def one(flag):
        return jnp.where(flag, 1, 0)

    rounds = (((2, 1), (2, -1), (-2, 1), (-2, -1), (0, 1), (0, -1)), ((4, 0), (-4, 0)))

    def inside(ds, dg):
        flag = sfc + ds < n_sfc if ds >= 0 else sfc + ds >= 0
        return jnp.logical_and(flag, grp + dg < n_grp if dg >= 0 else grp + dg >= 0)

    def tell(rnd):
        if gossip:
            for ds, dg in rounds[rnd]:
                @pl.when(inside(ds, dg))
                def _(ds=ds, dg=dg):
                    pl.semaphore_signal(
                        hello.at[rnd], inc=1, device_id={"sfc": sfc + ds, "grp": grp + dg},
                        device_id_type=MESH,
                    )

    def hear(rnd):
        if gossip:
            pl.semaphore_wait(hello.at[rnd], sum(one(inside(ds, dg)) for ds, dg in rounds[rnd]))

    lane = lax.broadcasted_iota(jnp.int32, (SUBS, LANES), 1)
    low_half = lane < LANES // 2

    def has(flag_int):
        return flag_int > 0

    has_below = one(sfc > 0)
    has_above = one(sfc < n_sfc - 1)
    has_left = one(grp > 0)
    has_right = one(grp < n_grp - 1)

    zero = jnp.zeros((SUBS, LANES), f32)
    for ref in (rhs, pre, gather, other):
        for t in range(wide):
            ref[t, pl.ds(0, SUBS), :] = zero
            ref[t, pl.ds(SUBS + rows, SUBS), :] = zero
    for t in range(wide):
        for ref in (coarse, ea, eb):
            ref[t, pl.ds(0, SUBS), :] = zero
            ref[t, pl.ds(SUBS + crows, SUBS), :] = zero
    for t in range(wide):
        for at in (SUBS, rows):
            other[t, pl.ds(at, SUBS), :] = zero

    source_copy.wait()

    def copies(e, ds, dg, src):
        gpos = 1 - dg
        if ds == 0:
            source, target = src, side.at[e, gpos // 2]
        else:
            tile, amount = ((0, 2), (1, 3), (3, 2))[dg + 1]
            source = packed.at[e, int(ds > 0), pl.ds(tile, amount)]
            target = (below if ds > 0 else above).at[e, gpos, pl.ds(0, amount)]
        return pltpu.make_async_remote_copy(
            src_ref=source, dst_ref=target, send_sem=trade_sem.at[0],
            recv_sem=trade_sem.at[1 if e == 0 else 2 if (dg, ds) < (0, 0) else 3], device_id={"sfc": sfc + ds, "grp": grp + dg},
            device_id_type=MESH,
        )

    def start(e, src):
        for ds, dg in WAYS:
            @pl.when(there(ds, dg))
            def _(ds=ds, dg=dg):
                copies(e, ds, dg, src).start()

    column = slots * edge * tiles // SUBS
    ends, layers = has_left + has_right, has_below + has_above

    def settle(sem, amounts, times=1):
        for flags, tiles_in in amounts:
            if tiles_in:
                @pl.when(functools.reduce(jnp.logical_and, flags))
                def _(tiles_in=tiles_in):
                    ref = dummy.at[pl.ds(0, times * tiles_in)]
                    pltpu.make_async_copy(ref, ref, trade_sem.at[sem]).wait()

    def half_of(beside, along):
        return [
            ((beside == b, along == a, layers == l), b * (column + 2 * l) + 3 * a)
            for b in (0, 1) for l in (0, 1, 2) for a in (0, 1) if l - 1 <= a <= l
        ]

    both = [((ends == b, layers == l), b * (column + 2 * l) + 3 * l) for b in range(3) for l in range(3)]
    high, low_end = half_of(has_right, has_above), half_of(has_left, has_below)

    def pack(e, src, columns=None):
        cut = SUBS // 2

        def layer(s, t):
            if columns is None:
                return src[pl.ds(s * edge, edge), pl.ds(t * LANES, LANES)]
            return columns[t][s * edge : (s + 1) * edge]

        for up in (0, 1):
            value = [layer(0, t) for t in range(tiles)]
            if up:
                for s in range(1, slots):
                    value = [jnp.where(count > s, layer(s, t), value[t]) for t in range(tiles)]
            if up:
                near = [v[edge - SUBS :] for v in value]
                far = [v[edge - SUBS - cut : edge - SUBS] for v in value]
                edges = [v[edge - cut :] for v in value]
            else:
                near = [v[:SUBS] for v in value]
                far = [v[SUBS : SUBS + cut] for v in value]
                edges = [v[:cut] for v in value]
            packed[e, up, 0] = jnp.concatenate([far[0], edges[1]], axis=0)
            packed[e, up, 1] = near[0]
            packed[e, up, 2] = jnp.concatenate([far[0], far[1]], axis=0)
            packed[e, up, 3] = near[1]
            packed[e, up, 4] = jnp.concatenate([far[1], edges[0]], axis=0)

    def ghost(ref, e, up, g, h, t):
        cut = SUBS // 2
        near_h = 1 if up else 0
        if g == 1:
            if h == near_h:
                return ref[e, g, 0 if t == 0 else 2]
            mix, low = ref[e, g, 1], t == 0
        else:
            full = 1 if g == 0 else 0
            if h == near_h and t == full:
                return ref[e, g, 0 if g == 0 else 1]
            mix = ref[e, g, 1 if g == 0 else 0]
            if h == near_h:
                low = False
            elif t == full:
                low = True
            else:
                return jnp.zeros((SUBS, LANES), f32)
        part = mix[:cut] if low else mix[cut:]
        none = jnp.zeros((cut, LANES), f32)
        return jnp.concatenate([none, part] if up else [part, none], axis=0)

    def unpack(e, src):
        sides = ((0, has_left), (1, 1), (2, has_right))
        for g, present in sides:
            for s in range(slots + 2):
                for h in range(edge // SUBS):
                    for t in range(tiles):
                        cols = pl.ds(t * LANES, LANES)

                        def centre(slot):
                            at = pl.ds(slot * edge + h * SUBS, SUBS)
                            return src[at, cols] if g == 1 else side[e, g // 2, at, cols]

                        if s == 0:
                            value = jnp.where(has(has_below * present), ghost(below, e, 1, g, h, t), 0.0)
                        else:
                            up = one(count == s - 1) * has_above * present
                            value = jnp.zeros((SUBS, LANES), f32)
                            if s >= 2:
                                value = jnp.where(has(up), ghost(above, e, 0, g, h, t), value)
                            if s <= slots:
                                value = jnp.where(has(one(count >= s) * present), centre(s - 1), value)
                        rhs[g * tiles + t, pl.ds(SUBS + s * edge + h * SUBS, SUBS), :] = value

    def body(ref, t, first=0, n=rows):
        return ref[t, pl.ds(SUBS + first, n), :]

    def around(ref, t, first=0, n=rows):
        return ref[t, pl.ds(SUBS + first - 1, n), :] + ref[t, pl.ds(SUBS + first + 1, n), :]

    def spot(t):
        return t // tiles

    def product(values, pieces, at, width):
        n = values[0].shape[0]
        parts = [split(v, pieces) for v in values]
        lhs = jnp.concatenate([jnp.concatenate(p, axis=1) for p in parts], axis=0)
        w = weight_ref[pl.ds(0, pieces * LANES), pl.ds(at, width)]
        out = jnp.dot(lhs, w, preferred_element_type=f32)

        def get(i, k):
            return out[i * n : (i + 1) * n, k * LANES : (k + 1) * LANES]

        return get

    def halves(n):
        return jnp.broadcast_to(low_half[:1], (n, LANES))

    def cross(get, i, k, k_up, count_, n):
        none = jnp.zeros((n, LANES), f32)
        lower = get(i - 1, k_up) if 0 < i <= count_ else none
        upper = get(i + 1, k) if -1 <= i < count_ - 1 else none
        return lower, upper

    def blend(get, i, k, amount, n):
        lower, upper = cross(get, i, k, k, amount, n)
        return jnp.where(halves(n), lower, upper)

    low_wall = jnp.where(jnp.logical_and(lane < edge, grp == 0), 1.0, 0.0)
    high_wall = jnp.where(jnp.logical_and(lane >= LANES - edge, grp == n_grp - 1), 1.0, 0.0)

    def walls(value, x, t):
        n = value.shape[0]
        if t == mine[0]:
            value = value - x * jnp.broadcast_to(low_wall[:1], (n, LANES))
        if t == mine[-1]:
            value = value - x * jnp.broadcast_to(high_wall[:1], (n, LANES))
        return value

    def smooth():
        get = product([body(rhs, t) for t in range(wide)], 2, 0, 4 * LANES)
        seconds = []
        for t in range(wide):
            r = body(rhs, t)
            first = get(t, 0) + blend(get, t, 1, wide, rows)
            seconds.append(walls(get(t, 2) + blend(get, t, 3, wide, rows), r, t))
            near = around(rhs, t)
            if t in mids:
                pre[t, pl.ds(SUBS, rows), :] = 9.0 * r + near + 0.5 * first
            gather[t, pl.ds(SUBS, rows), :] = mask[1] * (first + near)
        for t in range(wide):
            other[t, pl.ds(SUBS, rows), :] = seconds[t] + around(gather, t)

    def reflect(q, high):
        turned = pltpu.roll(q, LANES // 2, 1)
        n = q.shape[0]
        at = lax.broadcasted_iota(jnp.int32, (n, LANES), 1) // (2 * edge)
        near, far = (1, 2) if high else (2, 1)
        return jnp.where(at == near, -turned, jnp.where(at == far, -q, 0.0))

    def correct():
        qs = []
        for t in range(wide):
            q = (
                other[t, pl.ds(SUBS, crows, stride=2), :] + other[t, pl.ds(SUBS + 1, crows, stride=2), :]
            )
            qs.append(cmask[spot(t)] * q)
        left, right = mids[0], mids[-1]
        qs[left] = jnp.where(has(has_left), qs[left], reflect(qs[mine[0]], False))
        qs[right] = jnp.where(has(has_right), qs[right], reflect(qs[mine[-1]], True))
        powers = product([qs[t] for t in mids], 2, 4 * LANES, 4 * LANES)
        sides = product(qs, 2, 8 * LANES, 4 * LANES)

        def get(i, k):
            return powers(i - mids[0], k) if k < 4 else sides(i, k - 4)

        b0, b1, b2 = {}, {}, {}
        for t in mids:
            c = get(t, 0)
            j1 = get(t, 1) + blend(get, t, 4, wide, crows)
            j2 = get(t, 2) + blend(get, t, 5, wide, crows)
            j3 = get(t, 3) + (get(t - 1, 7) + get(t + 1, 6))
            coarse[t, pl.ds(SUBS, crows), :] = c
            b0[t] = 729.0 * c + 81.0 * j1 + (9.0 * j2 + j3)
            b1[t] = 81.0 * c + 18.0 * j1 + 3.0 * j2
            b2[t] = 9.0 * c + 3.0 * j1
        for t in mids:
            ea[t, pl.ds(SUBS, crows), :] = cmask[1] * (b2[t] + around(coarse, t, 0, crows))
        for t in mids:
            eb[t, pl.ds(SUBS, crows), :] = cmask[1] * (b1[t] + around(ea, t, 0, crows))
        return {t: b0[t] + around(eb, t, 0, crows) for t in mids}

    scale = CSTEP * STEP * STEP * STEP / 8.0
    square = STEP * STEP

    def finish(e, outs, low, n):
        for t in mids:
            for up in (0, 1):
                gather[t, pl.ds(SUBS + up, crows, stride=2), :] = e[t]
        for t in mids:
            other[t, pl.ds(SUBS + low, n), :] = mask[spot(t), pl.ds(low, n), :] * (
                body(pre, t, low, n) + scale * body(gather, t, low, n)
            )
        get = product([body(other, t, low, n) for t in mids], 3, 0, 4 * LANES)
        first, out = mids[0], {}
        near = len(mids)
        for t in outs:
            i = t - first
            if t in mids:
                value = get(i, 0) + blend(get, i, 1, near, n) + around(other, t, low, n)
            else:
                value = blend(get, i, 1, near, n)
            gather[t, pl.ds(SUBS + low, n), :] = mask[1, pl.ds(low, n), :] * value
        for t in outs:
            i = t - first
            second = blend(get, i, 3, near, n)
            if t in mids:
                second = walls(get(i, 2) + second, body(other, t, low, n), t)
            out[t] = square * (second + around(gather, t, low, n))
            if t in mids:
                out[t] = body(pre, t, low, n) + out[t]
        return out

    def owned(out, low):
        return [own[...] * out[t][edge - low : edge - low + planes] for t in mine]

    def laplace():
        lanes = lax.broadcasted_iota(jnp.int32, (planes, LANES), 1)
        z = lanes % edge
        tile = {t: body(gather, t, edge, planes) for t in mids}
        ahead = {t: pltpu.roll(tile[t], LANES - edge, 1) for t in mids[1:]}
        behind = {t: pltpu.roll(tile[t], edge, 1) for t in mids[:-1]}
        out = []
        for t in mine:
            v = tile[t]
            beside = jnp.where(z < edge - 1, pltpu.roll(v, LANES - 1, 1), 0.0)
            beside = beside + jnp.where(z > 0, pltpu.roll(v, 1, 1), 0.0)
            beside = beside + jnp.where(lanes < LANES - edge, ahead[t], ahead[t + 1])
            beside = beside + jnp.where(lanes >= edge, behind[t], behind[t - 1])
            out.append(square * (own[...] * (6.0 * v - around(gather, t, edge, planes) - beside)))
        return out

    count = count_hbm[0]
    pack(0, source_ref)
    if gossip:
        near = (1 + one(sfc > 0) + one(sfc < n_sfc - 1)) * (1 + one(grp > 0) + one(grp < n_grp - 1))
        pl.semaphore_wait(barrier, near - 1)
    else:
        pl.semaphore_wait(barrier, everyone - 1)
    start(0, source_ref)

    for g, present in enumerate((has_left, 1, has_right)):
        for s in range(slots + 2):
            if s == 0:
                ok = has_below
            else:
                ok = one(count >= s) + one(count == s - 1) * has_above
            value = jnp.full((SUBS, LANES), ok * present, jnp.int32).astype(f32)
            for h in range(edge // SUBS):
                mask[g, pl.ds(s * edge + h * SUBS, SUBS), :] = value
            for h in range(half // SUBS):
                cmask[g, pl.ds(s * half + h * SUBS, SUBS), :] = value
    for s in range(slots):
        value = jnp.full((SUBS, LANES), one(count > s), jnp.int32).astype(f32)
        for h in range(edge // SUBS):
            own[pl.ds(s * edge + h * SUBS, SUBS), :] = value
    pltpu.make_async_copy(weight_ref, weight_ref, local_sem.at[1]).wait()

    settle(1, both)
    unpack(0, source_ref)
    smooth()
    tell(0)
    low, n = SUBS, rows - 2 * SUBS
    out = finish(correct(), mids, low, n)
    for t in mids:
        gather[t, pl.ds(SUBS + low, n), :] = mask[spot(t), pl.ds(low, n), :] * out[t]
    firsts = owned(out, low)
    images = laplace()
    for i, value in enumerate(images):
        image_buf[:, pl.ds(i * LANES, LANES)] = value
    pack(1, None, images)
    start(1, image_buf)
    hear(0)
    tell(1)
    acc_rz, acc_curv = zero, zero
    for i in range(tiles):
        cols = pl.ds(i * LANES, LANES)
        value = square * firsts[i]
        image = images[i]
        source = body(rhs, mine[i], edge, planes) * own[...]
        first_ref[:, cols] = value
        image_ref[:, cols] = image
        source_out[:, cols] = source
        acc_rz = acc_rz + jnp.sum((source * value).reshape(-1, SUBS, LANES), axis=0)
        acc_curv = acc_curv + jnp.sum((value * image).reshape(-1, SUBS, LANES), axis=0)
    row = lax.broadcasted_iota(jnp.int32, (1, LANES), 1)

    def whole(acc):
        return jnp.sum(jnp.sum(acc, axis=0, keepdims=True), axis=1, keepdims=True)

    rz, curv = whole(acc_rz), whole(acc_curv)
    known = jnp.where(row == 0, rz, jnp.where(row == 1, curv, 0.0))

    for t in range(wide):
        if t in mine:
            rhs[t, pl.ds(SUBS, edge), :] = jnp.zeros((edge, LANES), f32)
            rhs[t, pl.ds(SUBS + edge, planes), :] = images[t - tiles]
            rhs[t, pl.ds(SUBS + edge + planes, edge), :] = jnp.zeros((edge, LANES), f32)
        else:
            rhs[t, pl.ds(SUBS, rows), :] = jnp.zeros((rows, LANES), f32)
    smooth()
    out = finish(correct(), range(wide), 0, rows)
    for t in range(wide):
        dual[t] = mask[spot(t)] * out[t]
    acc = zero
    for t in mine:
        part_of = dual[t, pl.ds(edge, planes), :] * images[t - tiles]
        acc = acc + jnp.sum(part_of.reshape(-1, SUBS, LANES), axis=0)
    settle(2, high)
    pairs = zero
    for g, present in ((1, 1), (2, has_right)):
        for s in range(slots + 2):
            for h in range(edge // SUBS):
                for t in range(tiles):
                    if s == 0:
                        value = jnp.where(has(has_below * present), ghost(below, 1, 1, g, h, t), 0.0)
                    else:
                        value = zero
                        if s >= 2:
                            up = one(count == s - 1) * has_above * present
                            value = jnp.where(has(up), ghost(above, 1, 0, g, h, t), value)
                        if g == 2 and s <= slots:
                            at = pl.ds((s - 1) * edge + h * SUBS, SUBS)
                            centre = side[1, 1, at, pl.ds(t * LANES, LANES)]
                            value = jnp.where(has(one(count >= s) * present), centre, value)
                    if g == 2 or s >= 2:
                        pairs = pairs + dual[g * tiles + t, pl.ds(s * edge + h * SUBS, SUBS), :] * value
    acc = acc + 2.0 * pairs

    def send(slot, device):
        return pltpu.make_async_remote_copy(
            src_ref=part, dst_ref=red.at[slot], send_sem=red_sem.at[0],
            recv_sem=red_sem.at[1], device_id=device, device_id_type=MESH,
        )

    value = jnp.concatenate([square * jnp.sum(acc, axis=0, keepdims=True), known], axis=0)
    part[...] = value
    red[me] = value
    hear(1)

    if everyone <= 64:
        for i in range(n_sfc - 1):
            other_sfc = i + one(i >= sfc)
            for g in range(n_grp):
                send(me, {"sfc": other_sfc, "grp": g}).start()
        for i in range(n_grp - 1):
            send(me, {"sfc": sfc, "grp": i + one(i >= grp)}).start()
    else:
        def go(i, carry):
            peer, device = place(i)
            send(me, device).start()
            return carry

        lax.fori_loop(1, everyone, go, 0)
    settle(3, low_end)
    unpack(1, image_buf)
    smooth()
    for i, value in enumerate(owned(finish(correct(), mine, SUBS, rows - 2 * SUBS), SUBS)):
        w_ref[:, pl.ds(i * LANES, LANES)] = square * value
    settle(0, both, 2)

    rest = red.at[pl.ds(0, everyone - 1)]
    pltpu.make_async_copy(rest, rest, red_sem.at[0]).wait()
    pltpu.make_async_copy(rest, rest, red_sem.at[1]).wait()
    sums = red[...]
    while sums.shape[0] % 2 == 0:
        sums = sums[: sums.shape[0] // 2] + sums[sums.shape[0] // 2 :]
    sums = jnp.sum(sums, axis=0)

    def pick(value):
        return jnp.sum(value, axis=1, keepdims=True)

    rz = pick(jnp.where(row == 0, sums[1:], 0.0))
    inverse = 1.0 / pick(jnp.where(row == 1, sums[1:], 0.0))
    alpha = rz * inverse
    ratio = pick(sums[:1]) * inverse
    scale_ref[...] = jnp.concatenate(
        [jnp.broadcast_to(alpha, (1, LANES)), jnp.broadcast_to(ratio, (1, LANES))], axis=0
    )


def combine(first, image, w, source, scale, solution_ref, residual_ref, direction_ref):
    alpha = scale[0:1, 0:1]
    ratio = scale[1:2, 0:1]
    solution_ref[...] = alpha * first[...]
    residual_ref[...] = source[...] - alpha * image[...]
    direction_ref[...] = alpha * (ratio * first[...] - w[...])


def shards(n_sfc, n_grp, source, layer_counts):
    slots, edge, width = source.shape
    planes, tiles = slots * edge, width // LANES
    rows, crows = (slots + 2) * edge, (slots + 2) * edge // 2
    f32 = jnp.float32
    vmem = pltpu.VMEM
    dma = pltpu.SemaphoreType.DMA
    n = n_sfc * n_grp
    out = jax.ShapeDtypeStruct((planes, width), f32)
    fine = vmem((3 * tiles, rows + 2 * SUBS, LANES), f32)
    coarse = vmem((3 * tiles, crows + 2 * SUBS, LANES), f32)
    parts = pl.pallas_call(
        functools.partial(kernel, (slots, edge, tiles, n_sfc, n_grp)),
        out_shape=(out, out, out, out, jax.ShapeDtypeStruct((2, LANES), f32)),
        in_specs=[pl.BlockSpec(memory_space=pltpu.SMEM)] + [pl.BlockSpec(memory_space=pltpu.HBM)] * 2,
        out_specs=[pl.BlockSpec(memory_space=pltpu.VMEM)] * 5,
        scratch_shapes=[
            vmem((planes, width), f32),
            vmem((planes, width), f32),
            vmem((3 * LANES, 12 * LANES), jnp.bfloat16),
            fine, fine, fine, fine,
            vmem((3 * tiles, rows, LANES), f32),
            coarse, coarse, coarse,
            vmem((3, rows, LANES), f32),
            vmem((3, crows, LANES), f32),
            vmem((planes, LANES), f32),
            vmem((2, 2, 5, SUBS, LANES), f32),
            vmem((2, 2, planes, width), f32),
            vmem((2, 3, 3, SUBS, LANES), f32),
            vmem((2, 3, 3, SUBS, LANES), f32),
            vmem((2, LANES), f32),
            vmem((n, 2, LANES), f32),
            vmem((4 * planes * tiles // SUBS + 28, SUBS, LANES), f32),
            dma((2,)),
            dma((4,)),
            dma((2,)),
            pltpu.SemaphoreType.REGULAR((2,)),
        ],
        compiler_params=pltpu.CompilerParams(
            collective_id=0, has_side_effects=True, vmem_limit_bytes=16 * 1024 * 1024
        ),
        name="pcg",
    )(layer_counts, pltpu.with_memory_space_constraint(source.reshape(planes, width), pltpu.HBM), pltpu.with_memory_space_constraint(jnp.asarray(weights(edge)), pltpu.HBM))
    outs = pl.pallas_call(
        combine,
        out_shape=(out, out, out),
        in_specs=[pl.BlockSpec(memory_space=pltpu.VMEM)] * 5,
        out_specs=[pl.BlockSpec(memory_space=pltpu.VMEM)] * 3,
        compiler_params=pltpu.CompilerParams(vmem_limit_bytes=16 * 1024 * 1024),
        name="combine",
    )(*parts)
    return tuple(o.reshape(source.shape) for o in outs)


def solution(mesh):
    n_sfc, n_grp = mesh.shape["sfc"], mesh.shape["grp"]
    return jax.shard_map(
        functools.partial(shards, n_sfc, n_grp),
        mesh=mesh,
        in_specs=(P("sfc", None, "grp"), P("sfc")),
        out_specs=(P("sfc", None, "grp"), P("sfc", None, "grp"), P("sfc", None, "grp")),
        check_vma=False,
    )
```
